128 devices in a mesh: dp: 8 (over x, core), tensor: 8 (over y_lo, z), section: 2 (over y_hi).
Axes of the slice: x: 4, y: 4 (y_hi: 2, y_lo: 2; y = y_hi * 2 + y_lo), z: 4, core: 2. Of those that a mesh axis runs over, the one named last changes fastest.
Arguments:
- patches: bfloat16 [32, 256, 1152], P(('dp', 'section'), 'tensor'), may hold values from -6 to 6
- teacher: int32 [32, 7], P(('dp', 'section')), may hold values from 0 to 255
- proj_w: bfloat16 [1152, 4096], P(None, ('dp', 'tensor', 'section')), may hold values from -0.1875 to 0.1875
- norm_gain: bfloat16 [4096], replicated, may hold values from 0.25 to 1.75
- wq: bfloat16 [4096, 4096], P(('dp', 'section'), 'tensor'), may hold values from -0.09375 to 0.09375
- wk: bfloat16 [4096, 4096], P(('dp', 'section'), 'tensor'), may hold values from -0.09375 to 0.09375
- wv: bfloat16 [4096, 4096], P(('dp', 'section'), 'tensor'), may hold values from -0.09375 to 0.09375
- wo: bfloat16 [4096, 4096], P('tensor', ('dp', 'section')), may hold values from -0.09375 to 0.09375
- start_row: bfloat16 [4096], replicated, may hold values from -6 to 6
- action_table: bfloat16 [256, 4096], replicated, may hold values from -6 to 6
- final_gain: bfloat16 [4096], replicated, may hold values from 0.25 to 1.75
- head_w: bfloat16 [4096, 256], replicated, may hold values from -0.25 to 0.25
Outputs:
- hidden_out: bfloat16 [32, 256, 4096], P(('dp', 'section'), 'tensor')
- loss: float32 [32, 7], P(('dp', 'section'))
The draws below stay inside these ranges and needn't reach their ends.
All inputs are finite; a program needn't handle non-finite values.
Results may differ from the reference program's by a relative error of at most 0.0054.
Values may be sent and summed in bfloat16 or wider, within the bound.
No kernel may reach another device: no remote copies, remote signals or barrier semaphores. Data moves between devices by JAX's collectives and lax.ppermute only.
A program may use at most 128 MiB of HBM per device.

```python
import math
import jax
import jax.numpy as jnp
from jax import lax

D = 4096
HEADS = 32
HD = 128
V = 1152
P_SIZE = 256
BINS = 256
ADIM = 7
SLOTS = 8
FRAMES = 32


def touch_ends(values, rng, low, largest):
    place = [jax.random.randint(jax.random.fold_in(rng, axis), (), 0, length) for axis, length in enumerate(values.shape)]
    main_axis = values.shape.index(max(values.shape))
    beside = place[:main_axis] + [(place[main_axis] + 1) % values.shape[main_axis]] + place[main_axis + 1:]
    return values.at[tuple(place)].set(low).at[tuple(beside)].set(largest)


def shard_levels(rng, shape, pieces, smallest, largest):
    def one(axis_at, blocks):
        heights = jax.random.uniform(jax.random.fold_in(jax.random.fold_in(rng, 6), axis_at), (blocks,), jnp.float32, smallest / len(pieces), largest / len(pieces))
        return jnp.repeat(jnp.exp(heights), shape[axis_at] // blocks).reshape((-1,) + (1,) * (len(shape) - axis_at - 1))

    loudness = one(*pieces[0])
    for cut in pieces[1:]:
        loudness = loudness * one(*cut)
    return loudness


def scatter_about(own_key, shape, deviation, reach, cuts=(), kind=jnp.bfloat16):
    array = jax.random.normal(own_key, shape, jnp.float32) * deviation
    if len(cuts) > 0:
        array = shard_levels(own_key, shape, cuts, -0.22, 0.18) * array
    return jnp.clip(array, min=-reach, max=reach).astype(kind)


def setup_inputs(seed: int = 0) -> dict:
    splits = jax.random.split(jax.random.key(seed), 13)
    return {
        "patches": scatter_about(splits[0], (FRAMES, P_SIZE, V), 1.0, 6.0, ((0, 16), (1, 8))),
        "teacher": touch_ends(jax.random.randint(splits[1], (FRAMES, ADIM), 0, BINS), jax.random.fold_in(splits[1], 1), 0, BINS - 1).astype(jnp.int32),
        "proj_w": scatter_about(splits[2], (V, D), V ** -0.5, 0.1875, ((1, 128),)),
        "norm_gain": jnp.clip(1.0 + 0.15 * jax.random.normal(splits[3], (D,), jnp.float32), 0.25, 1.75).astype(jnp.bfloat16),
        "wq": scatter_about(splits[4], (D, D), D ** -0.5, 0.09375, ((0, 16), (1, 8))),
        "wk": scatter_about(splits[5], (D, D), D ** -0.5, 0.09375, ((0, 16), (1, 8))),
        "wv": scatter_about(splits[6], (D, D), D ** -0.5, 0.09375, ((0, 16), (1, 8))),
        "wo": scatter_about(splits[7], (D, D), D ** -0.5, 0.09375, ((0, 8), (1, 16))),
        "start_row": scatter_about(splits[8], (D,), 1.0, 6.0),
        "action_table": scatter_about(splits[9], (BINS, D), 1.0, 6.0),
        "final_gain": jnp.clip(1.0 + 0.15 * jax.random.normal(splits[10], (D,), jnp.float32), 0.25, 1.75).astype(jnp.bfloat16),
        "head_w": scatter_about(splits[11], (D, BINS), (D // 9) ** -0.5, 0.25),
    }


eps = 1e-05

def normalize(rows, gain):
    rows = rows.astype(jnp.float32)
    factor = lax.rsqrt(lax.optimization_barrier(jnp.mean(rows * rows, axis=-1, keepdims=True)) + eps)
    return rows * factor * gain.astype(jnp.float32)

def action_rows(teacher, start_row, action_table):
    frames = teacher.shape[0]
    onehot = (teacher[..., None] == jnp.arange(BINS, dtype=jnp.int32)).astype(jnp.bfloat16)
    looked = jnp.dot(onehot.reshape(-1, BINS), action_table, preferred_element_type=jnp.float32)
    looked = looked.astype(jnp.bfloat16).reshape(frames, ADIM, D)
    start = jnp.broadcast_to(start_row.reshape(1, 1, D), (frames, 1, D))
    return jnp.concatenate([start, looked], axis=1)

def reference(patches, teacher, proj_w, norm_gain, wq, wk, wv, wo, start_row, action_table, final_gain, head_w):
    frames = patches.shape[0]
    length = P_SIZE + SLOTS
    embedded = jnp.dot(patches.reshape(-1, V), proj_w, preferred_element_type=jnp.float32)
    embedded = embedded.astype(jnp.bfloat16).reshape(frames, P_SIZE, D)
    actions = action_rows(teacher, start_row, action_table)
    stream = jnp.concatenate([embedded, actions], axis=1)
    normed = normalize(stream, norm_gain).astype(jnp.bfloat16).reshape(-1, D)
    queries = jnp.dot(normed, wq, preferred_element_type=jnp.float32).astype(jnp.bfloat16).reshape(frames, length, HEADS, HD)
    keys_all = jnp.dot(normed, wk, preferred_element_type=jnp.float32).astype(jnp.bfloat16).reshape(frames, length, HEADS, HD)
    values_all = jnp.dot(normed, wv, preferred_element_type=jnp.float32).astype(jnp.bfloat16).reshape(frames, length, HEADS, HD)
    positions = jnp.arange(length, dtype=jnp.int32)
    causal = positions[:, None] >= positions[None, :]
    inv_root = 1.0 / math.sqrt(HD)

    def one_frame(items):
        query_f, key_f, value_f = items
        scores = jnp.einsum('qhd,khd->hqk', query_f.astype(jnp.float32), key_f.astype(jnp.float32)) * inv_root
        scores = jnp.where(causal[None], scores, -1e+30)
        weights = jax.nn.softmax(scores, axis=-1).astype(jnp.bfloat16)
        result = jnp.einsum('hqk,khd->qhd', weights.astype(jnp.float32), value_f.astype(jnp.float32))
        return result.astype(jnp.bfloat16)
    mixed = lax.map(one_frame, (queries, keys_all, values_all)).reshape(-1, D)
    update = jnp.dot(mixed, wo, preferred_element_type=jnp.float32).reshape(frames, length, D)
    hidden_out = (embedded.astype(jnp.float32) + update[:, :P_SIZE]).astype(jnp.bfloat16)
    acted = actions[:, :ADIM].astype(jnp.float32) + update[:, P_SIZE:P_SIZE + ADIM]
    final = normalize(acted, final_gain).astype(jnp.bfloat16).reshape(-1, D)
    logits = jnp.dot(final, head_w, preferred_element_type=jnp.float32).reshape(frames, ADIM, BINS)
    chosen = (teacher[..., None] == jnp.arange(BINS, dtype=jnp.int32)).astype(jnp.float32)
    picked = lax.optimization_barrier(jnp.sum(logits * chosen, axis=-1))
    loss = jax.nn.logsumexp(logits, axis=-1) - picked
    return (hidden_out, loss)
```

```python
import math

import jax
import jax.numpy as jnp
import numpy as np
from jax import lax
from jax.experimental import pallas as pl
from jax.experimental.pallas import tpu as pltpu
from jax.sharding import PartitionSpec as P

D = 4096
HD = 128
V = 1152
P_SIZE = 256
BINS = 256
ADIM = 7
SLOTS = 8
FRAMES = 2
ROWS = FRAMES * P_SIZE
ACTS = FRAMES * SLOTS
HEADS = 4
NB = 16

eps = 1e-05


AXES = ("dp", "tensor", "section")
IDS = np.arange(128).reshape(4, 2, 2, 4, 2)
VMEM = pl.BlockSpec(memory_space=pltpu.VMEM)
SMEM = pl.BlockSpec(memory_space=pltpu.SMEM)
ANY = pl.BlockSpec(memory_space=pl.ANY)
LIMIT = pltpu.CompilerParams(vmem_limit_bytes=56 * 1024 * 1024)


def get(s, dx=0, dc=0, dyl=0, dz=0, dyh=0):
    pairs = []
    for x, c, yl, z, yh in np.ndindex(IDS.shape):
        source = IDS[(x + dx) % 4, c ^ dc, yl ^ dyl, (z + dz) % 4, yh ^ dyh]
        pairs.append((int(source), int(IDS[x, c, yl, z, yh])))
    return lax.ppermute(s, AXES, pairs)


def weight_pieces(shard):
    near = (shard, get(shard, dyh=1))
    ahead = tuple(get(s, dx=1) for s in near)
    behind = tuple(get(s, dx=3) for s in near)
    across = (get(ahead[0], dx=1), get(behind[1], dx=3))
    rings = (near, ahead, across, behind)
    pieces = []
    for ring in rings:
        pieces += list(ring)
        pieces += [get(s, dc=1) for s in ring]
    return pieces


def normalize(rows, gain):
    rows = rows.astype(jnp.float32)
    factor = lax.rsqrt(jnp.mean(rows * rows, axis=-1, keepdims=True) + eps)
    return rows * factor * gain.astype(jnp.float32)


def action_rows(teacher, start_row, action_table):
    frames = teacher.shape[0]
    onehot = (teacher[..., None] == jnp.arange(BINS, dtype=jnp.int32)).astype(jnp.bfloat16)
    looked = jnp.dot(onehot.reshape(-1, BINS), action_table, preferred_element_type=jnp.float32)
    looked = looked.astype(jnp.bfloat16).reshape(frames, ADIM, D)
    start = jnp.broadcast_to(start_row.reshape(1, 1, D), (frames, 1, D))
    return jnp.concatenate([start, looked], axis=1)


def norm_kernel(slot_ref, nb_ref, gain_ref, act_ref, *refs):
    blocks, (out_ref, emb_ref, all_ref, sems) = refs[:8], refs[8:]
    copies = [
        pltpu.make_async_copy(blocks[r], all_ref.at[slot_ref[r]], sems.at[r]) for r in range(8)
    ]
    for copy in copies:
        copy.start()
    out_ref[:, ROWS : ROWS + ACTS, :] = act_ref[...]
    for copy in copies:
        copy.wait()
    step = 32
    low = lax.broadcasted_iota(jnp.int32, (step, 128), 1) < 64

    def chunk(i, carry):
        rows = pl.ds(pl.multiple_of(i * step, step), step)
        total = jnp.zeros((step, 128), jnp.float32)
        for t in range(8):
            for m in range(4):
                v = all_ref[t, rows, m * 128 : (m + 1) * 128].astype(jnp.float32)
                total = total + v * v
        mean = jnp.sum(total, axis=1, keepdims=True) * (1.0 / D)
        factor = lax.rsqrt(mean + eps)
        for ylo in range(2):
            for pair in range(2):
                for m in range(4):
                    cols = slice(m * 128, (m + 1) * 128)
                    a = all_ref[ylo * 4 + pair * 2, rows, cols].astype(jnp.float32)
                    b = all_ref[ylo * 4 + pair * 2 + 1, rows, cols].astype(jnp.float32)
                    even = jnp.where(low, a, pltpu.roll(b, 64, 1))
                    odd = jnp.where(low, pltpu.roll(a, 64, 1), b)
                    at = slice(pair * 128, (pair + 1) * 128)
                    for kc, v in ((2 * m, even), (2 * m + 1, odd)):
                        nb = nb_ref[kc] * 2 + ylo
                        emb_ref[nb, rows, at] = v.astype(jnp.bfloat16)
                        g = gain_ref[nb, :, at]
                        out_ref[nb, rows, at] = (v * factor * g).astype(jnp.bfloat16)
        return carry

    lax.fori_loop(0, ROWS // step, chunk, 0)


def norm_and_place(slots, kcs, gain, acts, blocks):
    return pl.pallas_call(
        norm_kernel,
        in_specs=[SMEM, SMEM, VMEM, VMEM] + [ANY] * 8,
        out_specs=[VMEM, VMEM],
        out_shape=[
            jax.ShapeDtypeStruct((NB, ROWS + ACTS, 256), jnp.bfloat16),
            jax.ShapeDtypeStruct((NB, ROWS, 256), jnp.bfloat16),
        ],
        scratch_shapes=[pltpu.VMEM((8, ROWS, 512), jnp.bfloat16), pltpu.SemaphoreType.DMA((8,))],
        compiler_params=LIMIT,
        name="norm_place",
    )(slots, kcs, gain, acts, *blocks)


def project_kernel(nb_ref, normed_ref, *refs):
    pieces, out_ref = refs[:16], refs[16]
    acc = None
    for p in range(16):
        part = jnp.dot(normed_ref[nb_ref[p]], pieces[p][...], preferred_element_type=jnp.float32)
        acc = part if acc is None else acc + part
    out_ref[...] = acc.astype(jnp.bfloat16)


def project(nbs, normed, pieces):
    width = pieces[0].shape[1]
    tile = 512
    return pl.pallas_call(
        project_kernel,
        grid=(width // tile,),
        in_specs=[SMEM, pl.BlockSpec(normed.shape, lambda n: (0, 0, 0))]
        + [pl.BlockSpec((256, tile), lambda n: (0, n))] * 16,
        out_specs=pl.BlockSpec((ROWS + ACTS, tile), lambda n: (0, n)),
        out_shape=jax.ShapeDtypeStruct((ROWS + ACTS, width), jnp.bfloat16),
        compiler_params=LIMIT,
        name="project",
    )(nbs, normed, *pieces)


def attend_kernel(qkv_ref, out_ref):
    inv_root = 1.0 / math.sqrt(HD)
    width = HEADS * HD
    causal = lax.broadcasted_iota(jnp.int32, (P_SIZE, P_SIZE), 0) >= lax.broadcasted_iota(
        jnp.int32, (P_SIZE, P_SIZE), 1
    )
    row_frame = lax.broadcasted_iota(jnp.int32, (ACTS, P_SIZE), 0) // SLOTS
    i = lax.broadcasted_iota(jnp.int32, (ACTS, ACTS), 0)
    j = lax.broadcasted_iota(jnp.int32, (ACTS, ACTS), 1)
    seen = (i // SLOTS == j // SLOTS) & (j <= i)

    def patch_rows(frame, start):
        return jnp.concatenate(
            [
                qkv_ref[t * 64 + frame * 32 : t * 64 + frame * 32 + 32, start : start + HD]
                for t in range(8)
            ],
            axis=0,
        )

    def scores(a, b):
        s = lax.dot_general(a, b, (((1,), (1,)), ((), ())), preferred_element_type=jnp.float32)
        return s * inv_root

    for h in range(HEADS):
        at = h * HD
        keys = [patch_rows(f, width + at) for f in range(FRAMES)]
        values = [patch_rows(f, 2 * width + at) for f in range(FRAMES)]
        for f in range(FRAMES):
            s = jnp.where(causal, scores(patch_rows(f, at), keys[f]), -1e30)
            e = jnp.exp(s - jnp.max(s, axis=-1, keepdims=True))
            w = (e / jnp.sum(e, axis=-1, keepdims=True)).astype(jnp.bfloat16)
            o = jnp.dot(w, values[f], preferred_element_type=jnp.float32).astype(jnp.bfloat16)
            for t in range(8):
                out_ref[t * 64 + f * 32 : t * 64 + f * 32 + 32, at : at + HD] = o[
                    t * 32 : (t + 1) * 32
                ]
        rows = slice(ROWS, ROWS + ACTS)
        qa = qkv_ref[rows, at : at + HD]
        ka = qkv_ref[rows, width + at : width + at + HD]
        va = qkv_ref[rows, 2 * width + at : 2 * width + at + HD]
        parts = [jnp.where(row_frame == f, scores(qa, keys[f]), -1e30) for f in range(FRAMES)]
        own = jnp.where(seen, scores(qa, ka), -1e30)
        top = jnp.max(own, axis=-1, keepdims=True)
        for s in parts:
            top = jnp.maximum(top, jnp.max(s, axis=-1, keepdims=True))
        parts = [jnp.exp(s - top) for s in parts]
        own = jnp.exp(own - top)
        total = jnp.sum(own, axis=-1, keepdims=True)
        for e in parts:
            total = total + jnp.sum(e, axis=-1, keepdims=True)
        mixed = jnp.dot(
            (own / total).astype(jnp.bfloat16), va, preferred_element_type=jnp.float32
        )
        for e, v in zip(parts, values):
            w = (e / total).astype(jnp.bfloat16)
            mixed = mixed + jnp.dot(w, v, preferred_element_type=jnp.float32)
        out_ref[rows, at : at + HD] = mixed.astype(jnp.bfloat16)


def attend(qkv):
    return pl.pallas_call(
        attend_kernel,
        in_specs=[VMEM],
        out_specs=VMEM,
        out_shape=jax.ShapeDtypeStruct((ROWS + ACTS, HEADS * HD), jnp.bfloat16),
        compiler_params=LIMIT,
        name="attend",
    )(qkv)


def expand_kernel(nb_ref, rel_ref, mixed_ref, *refs):
    pieces, (out_ref, act_ref) = refs[:16], refs[16:]
    mixed = mixed_ref[...]
    for p in range(16):
        acc = jnp.dot(mixed, pieces[p][...], preferred_element_type=jnp.float32)
        nb = nb_ref[p]
        for t in range(8):
            out_ref[rel_ref[t], nb] = acc[t * 64 : (t + 1) * 64].astype(jnp.bfloat16)
        act_ref[nb] = acc[ROWS : ROWS + ACTS].astype(jnp.bfloat16)


def expand(nbs, rels, mixed, pieces):
    return pl.pallas_call(
        expand_kernel,
        in_specs=[SMEM, SMEM, VMEM] + [VMEM] * 16,
        out_specs=[VMEM, VMEM],
        out_shape=[
            jax.ShapeDtypeStruct((8, NB, 64, 256), jnp.bfloat16),
            jax.ShapeDtypeStruct((NB, ACTS, 256), jnp.bfloat16),
        ],
        compiler_params=LIMIT,
        name="expand",
    )(nbs, rels, mixed, *pieces)


def on_device(
    patches, teacher, proj_w, norm_gain, wq, wk, wv, wo, start_row, action_table, final_gain, head_w
):
    dp = lax.axis_index("dp")
    tensor = lax.axis_index("tensor")
    x, core = dp // 2, dp % 2
    ylo, z = tensor // 4, tensor % 4
    yhi = lax.axis_index("section")

    k, c, j = np.meshgrid(np.arange(4), np.arange(2), np.arange(2), indexing="ij")
    kcs = ((x + k[:, :, 0]) % 4 * 2 + (core + c[:, :, 0]) % 2).reshape(-1).astype(jnp.int32)
    nbs = (kcs.reshape(4, 2, 1) * 2 + (yhi + j) % 2).reshape(-1).astype(jnp.int32)
    a, b = np.meshgrid(np.arange(2), np.arange(4), indexing="ij")
    slots = ((ylo + a) % 2 * 4 + (z + b) % 4).reshape(-1).astype(jnp.int32)
    rels = ((ylo + a) % 2 * 4 + (b - z) % 4).reshape(-1).astype(jnp.int32)

    shard = proj_w.T
    other = get(shard, dyh=1)
    first = yhi == 0
    both = jnp.concatenate([jnp.where(first, shard, other), jnp.where(first, other, shard)], axis=0)
    along = [both] + [get(both, dx=d) for d in (1, 2, 3)]
    columns = jnp.stack([jnp.stack([s, get(s, dc=1)]) for s in along]).reshape(512, V)

    own = patches.reshape(64, V)
    rows = lax.all_to_all(
        jnp.broadcast_to(own[None], (8, 64, V)), "tensor", 0, 0, tiled=True
    ).reshape(ROWS, V)

    qkv_pieces = weight_pieces(jnp.concatenate([wq, wk, wv], axis=1))
    wo_pieces = weight_pieces(wo)

    embedded = lax.dot_general(
        rows, columns, (((1,), (1,)), ((), ())), preferred_element_type=jnp.float32
    ).astype(jnp.bfloat16)
    pair = (embedded, get(embedded, dyl=1))
    up = tuple(get(e, dz=1) for e in pair)
    down = tuple(get(e, dz=3) for e in pair)
    far = (get(up[0], dz=1), get(down[1], dz=3))
    blocks = [r[i] for i in range(2) for r in (pair, up, far, down)]

    actions = action_rows(teacher, start_row, action_table)
    acts = normalize(actions, norm_gain).astype(jnp.bfloat16)
    acts = jnp.transpose(acts.reshape(ACTS, NB, 256), (1, 0, 2))
    gain = norm_gain.astype(jnp.float32).reshape(NB, 1, 256)
    normed, placed = norm_and_place(slots, kcs, gain, acts, blocks)
    embedded_own = lax.dynamic_slice_in_dim(placed, tensor * 64, 64, 1)

    mixed = attend(project(nbs, normed, qkv_pieces))
    product, act_product = expand(nbs, rels, mixed, wo_pieces)

    act_parts = jnp.transpose(act_product.reshape(NB, 8, 2, 256), (1, 2, 0, 3)).reshape(8, 2, D)
    act_parts = lax.all_to_all(act_parts, "tensor", 0, 0, tiled=True)
    act_update = jnp.sum(act_parts.astype(jnp.float32), axis=0)
    actions_own = lax.dynamic_slice_in_dim(actions.reshape(ACTS, D), tensor * 2, 2, 0)
    acted = actions_own.astype(jnp.float32) + act_update
    final = normalize(acted, final_gain).astype(jnp.bfloat16)
    logits = jnp.dot(final, head_w, preferred_element_type=jnp.float32)
    targets = jnp.pad(teacher, ((0, 0), (0, 1))).reshape(ACTS)
    target = lax.dynamic_slice_in_dim(targets, tensor * 2, 2, 0)
    chosen = (target[:, None] == jnp.arange(BINS, dtype=jnp.int32)).astype(jnp.float32)
    picked = jnp.sum(logits * chosen, axis=-1)
    loss_own = jax.nn.logsumexp(logits, axis=-1) - picked
    loss = lax.all_gather(loss_own, "tensor", axis=0, tiled=True).reshape(FRAMES, SLOTS)[:, :ADIM]

    update = product[0].astype(jnp.float32)
    for r in range(1, 8):
        part = get(product[r], dyl=r // 4, dz=-(r % 4))
        update = update + part.astype(jnp.float32)
    hidden = (embedded_own.astype(jnp.float32) + update).astype(jnp.bfloat16)
    hidden = jnp.transpose(hidden, (1, 0, 2)).reshape(FRAMES, 32, D)
    return (hidden, loss)


def solution(mesh):
    return jax.shard_map(
        on_device,
        mesh=mesh,
        in_specs=(
            P(("dp", "section"), "tensor", None),
            P(("dp", "section"), None),
            P(None, ("dp", "tensor", "section")),
            P(),
            P(("dp", "section"), "tensor"),
            P(("dp", "section"), "tensor"),
            P(("dp", "section"), "tensor"),
            P("tensor", ("dp", "section")),
            P(),
            P(),
            P(),
            P(),
        ),
        out_specs=(P(("dp", "section"), "tensor", None), P(("dp", "section"), None)),
        check_vma=False,
    )
```

```python
import math

import jax
import jax.numpy as jnp
import numpy as np
from jax import lax
from jax.experimental import pallas as pl
from jax.experimental.pallas import tpu as pltpu
from jax.sharding import PartitionSpec as P


D = 4096
HD = 128
V = 1152
P_SIZE = 256
BINS = 256
ADIM = 7
SLOTS = 8
FRAMES = 2
ROWS = FRAMES * P_SIZE
ACTS = FRAMES * SLOTS
HEADS = 4
SLOT, KC, BLOCK, REL, SIDE, OWN = 0, 8, 16, 32, 36, 38
NB = 16

eps = 1e-05


AXES = ("dp", "tensor", "section")
IDS = np.arange(128).reshape(4, 2, 2, 4, 2)
VMEM = pl.BlockSpec(memory_space=pltpu.VMEM)
SMEM = pl.BlockSpec(memory_space=pltpu.SMEM)
ANY = pl.BlockSpec(memory_space=pl.ANY)
LIMIT = pltpu.CompilerParams(vmem_limit_bytes=56 * 1024 * 1024)


def get(s, dx=0, dc=0, dyl=0, dz=0, dyh=0):
    pairs = []
    for x, c, yl, z, yh in np.ndindex(IDS.shape):
        source = IDS[(x + dx) % 4, c ^ dc, yl ^ dyl, (z + dz) % 4, yh ^ dyh]
        pairs.append((int(source), int(IDS[x, c, yl, z, yh])))
    return lax.ppermute(s, AXES, pairs)


def weight_pieces(shard):
    near = (shard, get(shard, dyh=1))
    ahead = tuple(get(s, dx=1) for s in near)
    behind = tuple(get(s, dx=3) for s in near)
    across = (get(ahead[0], dx=1), get(behind[1], dx=3))
    pieces = []
    for ring in (near, ahead, across, behind):
        pieces += list(ring)
        pieces += [get(s, dc=1) for s in ring]
    return pieces


def normalize(rows, gain):
    rows = rows.astype(jnp.float32)
    factor = lax.rsqrt(jnp.mean(rows * rows, axis=-1, keepdims=True) + eps)
    return rows * factor * gain.astype(jnp.float32)


def action_rows(teacher, start_row, action_table):
    frames = teacher.shape[0]
    onehot = (teacher[..., None] == jnp.arange(BINS, dtype=jnp.int32)).astype(jnp.bfloat16)
    looked = jnp.dot(onehot.reshape(-1, BINS), action_table, preferred_element_type=jnp.float32)
    looked = looked.astype(jnp.bfloat16).reshape(frames, ADIM, D)
    start = jnp.broadcast_to(start_row.reshape(1, 1, D), (frames, 1, D))
    return jnp.concatenate([start, looked], axis=1)


def project_kernel(table_ref, gain_ref, act_ref, *refs):
    blocks, pieces = refs[:8], refs[8:24]
    out_ref, emb_ref, all_ref, normed_ref, sems = refs[24:]
    step = 32
    low = lax.broadcasted_iota(jnp.int32, (step, 128), 1) < 64

    def placed(rows, store):
        for ylo in range(2):
            for pair in range(2):
                for m in range(4):
                    cols = slice(m * 128, (m + 1) * 128)
                    a = all_ref[ylo * 4 + pair * 2, rows, cols].astype(jnp.float32)
                    b = all_ref[ylo * 4 + pair * 2 + 1, rows, cols].astype(jnp.float32)
                    at = slice(pair * 128, (pair + 1) * 128)
                    even = jnp.where(low, a, pltpu.roll(b, 64, 1))
                    odd = jnp.where(low, pltpu.roll(a, 64, 1), b)
                    store(table_ref[KC + 2 * m] * 2 + ylo, at, even)
                    store(table_ref[KC + 2 * m + 1] * 2 + ylo, at, odd)

    def chunk(i, carry):
        rows = pl.ds(pl.multiple_of(i * step, step), step)
        totals = [jnp.zeros((step, 128), jnp.float32) for _ in range(4)]
        for t in range(8):
            for m in range(4):
                v = all_ref[t, rows, m * 128 : (m + 1) * 128].astype(jnp.float32)
                totals[m] = totals[m] + v * v
        total = (totals[0] + totals[1]) + (totals[2] + totals[3])
        mean = jnp.sum(total, axis=1, keepdims=True) * (1.0 / D)
        factor = jnp.broadcast_to(lax.rsqrt(mean + eps), (step, 128))

        def store(nb, at, v):
            normed_ref[nb, rows, at] = (v * factor * gain_ref[nb, :, at]).astype(jnp.bfloat16)

        placed(rows, store)
        return carry

    def own_chunk(i, carry):
        to = pl.ds(pl.multiple_of(i * step, step), step)

        def store(nb, at, v):
            emb_ref[nb, to, at] = v.astype(jnp.bfloat16)

        placed(pl.ds(pl.multiple_of(table_ref[OWN] * 64 + i * step, step), step), store)
        return carry

    @pl.when(pl.program_id(0) == 0)
    def _():
        copies = [
            pltpu.make_async_copy(blocks[r], all_ref.at[table_ref[SLOT + r]], sems.at[r])
            for r in range(8)
        ]
        for copy in copies:
            copy.start()
        normed_ref[:, ROWS : ROWS + ACTS, :] = act_ref[...]
        for copy in copies:
            copy.wait()
        lax.fori_loop(0, ROWS // step, chunk, 0)
        lax.fori_loop(0, 2, own_chunk, 0)

    acc = None
    for p in range(16):
        part = jnp.dot(
            normed_ref[table_ref[BLOCK + p]], pieces[p][...], preferred_element_type=jnp.float32
        )
        acc = part if acc is None else acc + part
    out_ref[...] = acc.astype(jnp.bfloat16)


def project(table, gain, acts, blocks, pieces):
    width = pieces[0].shape[1]
    tile = 512
    return pl.pallas_call(
        project_kernel,
        grid=(width // tile,),
        in_specs=[SMEM, VMEM, VMEM]
        + [ANY] * 8
        + [pl.BlockSpec((256, tile), lambda n: (0, n))] * 16,
        out_specs=[
            pl.BlockSpec((ROWS + ACTS, tile), lambda n: (0, n)),
            pl.BlockSpec((NB, 64, 256), lambda n: (0, 0, 0)),
        ],
        out_shape=[
            jax.ShapeDtypeStruct((ROWS + ACTS, width), jnp.bfloat16),
            jax.ShapeDtypeStruct((NB, 64, 256), jnp.bfloat16),
        ],
        scratch_shapes=[
            pltpu.VMEM((8, ROWS, 512), jnp.bfloat16),
            pltpu.VMEM((NB, ROWS + ACTS, 256), jnp.bfloat16),
            pltpu.SemaphoreType.DMA((8,)),
        ],
        compiler_params=LIMIT,
        name="project",
    )(table, gain, acts, *blocks, *pieces)


def attend_kernel(table_ref, qkv_ref, out_ref):
    inv_root = 1.0 / math.sqrt(HD)
    width = HEADS * HD
    half = P_SIZE // 2
    causal = [
        lax.broadcasted_iota(jnp.int32, (half, n), 0) + (n - half)
        >= lax.broadcasted_iota(jnp.int32, (half, n), 1)
        for n in (half, P_SIZE)
    ]
    row_frame = lax.broadcasted_iota(jnp.int32, (ACTS, P_SIZE), 0) // SLOTS
    i = lax.broadcasted_iota(jnp.int32, (ACTS, ACTS), 0)
    j = lax.broadcasted_iota(jnp.int32, (ACTS, ACTS), 1)
    seen = (i // SLOTS == j // SLOTS) & (j <= i)

    def patch_rows(frame, start):
        return jnp.concatenate(
            [
                qkv_ref[t * 64 + frame * 32 : t * 64 + frame * 32 + 32, start : start + HD]
                for t in range(8)
            ],
            axis=0,
        )

    def scores(a, b):
        s = lax.dot_general(a, b, (((1,), (1,)), ((), ())), preferred_element_type=jnp.float32)
        return s * inv_root

    for h in range(HEADS):
        at = h * HD
        keys = [patch_rows(f, width + at) for f in range(FRAMES)]
        values = [patch_rows(f, 2 * width + at) for f in range(FRAMES)]
        for f in range(FRAMES):
            queries = patch_rows(f, at)
            for i_half, n in enumerate((half, P_SIZE)):
                q = queries[i_half * half : (i_half + 1) * half]
                s = jnp.where(causal[i_half], scores(q, keys[f][:n]), -1e30)
                e = jnp.exp(s - jnp.max(s, axis=-1, keepdims=True))
                total = jnp.sum(e, axis=-1, keepdims=True)
                o = jnp.dot(
                    e.astype(jnp.bfloat16), values[f][:n], preferred_element_type=jnp.float32
                )
                o = (o * (1.0 / total)).astype(jnp.bfloat16)
                side = table_ref[SIDE + i_half]
                for t in range(4):
                    row = t * 64 + f * 32
                    out_ref[side, row : row + 32, at : at + HD] = o[t * 32 : (t + 1) * 32]
        rows = slice(ROWS, ROWS + ACTS)
        qa = qkv_ref[rows, at : at + HD]
        ka = qkv_ref[rows, width + at : width + at + HD]
        va = qkv_ref[rows, 2 * width + at : 2 * width + at + HD]
        parts = [jnp.where(row_frame == f, scores(qa, keys[f]), -1e30) for f in range(FRAMES)]
        own = jnp.where(seen, scores(qa, ka), -1e30)
        top = jnp.max(own, axis=-1, keepdims=True)
        for s in parts:
            top = jnp.maximum(top, jnp.max(s, axis=-1, keepdims=True))
        parts = [jnp.exp(s - top) for s in parts]
        own = jnp.exp(own - top)
        total = jnp.sum(own, axis=-1, keepdims=True)
        for e in parts:
            total = total + jnp.sum(e, axis=-1, keepdims=True)
        mixed = jnp.dot(own.astype(jnp.bfloat16), va, preferred_element_type=jnp.float32)
        for e, v in zip(parts, values):
            mixed = mixed + jnp.dot(
                e.astype(jnp.bfloat16), v, preferred_element_type=jnp.float32
            )
        mixed = mixed * (1.0 / total)
        for f in range(FRAMES):
            out_ref[table_ref[SIDE + f], 256:264, at : at + HD] = mixed[
                f * SLOTS : (f + 1) * SLOTS
            ].astype(jnp.bfloat16)


def attend(table, qkv):
    return pl.pallas_call(
        attend_kernel,
        in_specs=[SMEM, VMEM],
        out_specs=VMEM,
        out_shape=jax.ShapeDtypeStruct((2, 264, HEADS * HD), jnp.bfloat16),
        compiler_params=LIMIT,
        name="attend",
    )(table, qkv)


def expand_kernel(table_ref, own_ref, other_ref, *refs):
    pieces, (out_ref, act_ref) = refs[:16], refs[16:]
    own, other = own_ref[0], other_ref[...]
    for p in range(16):
        acc = jnp.dot(own, pieces[p][:512], preferred_element_type=jnp.float32)
        acc = acc + jnp.dot(other, pieces[p][512:], preferred_element_type=jnp.float32)
        nb = table_ref[BLOCK + p]
        for t in range(4):
            out_ref[table_ref[REL + t], nb] = acc[t * 64 : (t + 1) * 64].astype(jnp.bfloat16)
        act_ref[nb] = acc[256:264].astype(jnp.bfloat16)


def expand(table, mixed, other, pieces):
    return pl.pallas_call(
        expand_kernel,
        in_specs=[SMEM, VMEM, VMEM] + [VMEM] * 16,
        out_specs=[VMEM, VMEM],
        out_shape=[
            jax.ShapeDtypeStruct((4, NB, 64, 256), jnp.bfloat16),
            jax.ShapeDtypeStruct((NB, 8, 256), jnp.bfloat16),
        ],
        compiler_params=LIMIT,
        name="expand",
    )(table, mixed, other, *pieces)


def on_device(
    patches, teacher, proj_w, norm_gain, wq, wk, wv, wo, start_row, action_table, final_gain, head_w
):
    dp = lax.axis_index("dp")
    tensor = lax.axis_index("tensor")
    x, core = dp // 2, dp % 2
    ylo, z = tensor // 4, tensor % 4
    yhi = lax.axis_index("section")

    k, c, j = np.meshgrid(np.arange(4), np.arange(2), np.arange(2), indexing="ij")
    kcs = ((x + k[:, :, 0]) % 4 * 2 + (core + c[:, :, 0]) % 2).reshape(-1).astype(jnp.int32)
    nbs = (kcs.reshape(4, 2, 1) * 2 + (yhi + j) % 2).reshape(-1).astype(jnp.int32)
    a, b = np.meshgrid(np.arange(2), np.arange(4), indexing="ij")
    slots = ((ylo + a) % 2 * 4 + (z + b) % 4).reshape(-1).astype(jnp.int32)
    rels = ((np.arange(4) - z) % 4).astype(jnp.int32)
    sides = ((np.arange(2) + ylo) % 2).astype(jnp.int32)
    index = tensor.astype(jnp.int32).reshape(1)
    table = jnp.concatenate([slots, kcs, nbs, rels, sides, index])

    actions = action_rows(teacher, start_row, action_table)
    acts = normalize(actions, norm_gain).astype(jnp.bfloat16)
    acts = jnp.transpose(acts.reshape(ACTS, NB, 256), (1, 0, 2))
    gain = norm_gain.astype(jnp.float32).reshape(NB, 1, 256)
    actions_own = lax.dynamic_slice_in_dim(actions.reshape(ACTS, D), tensor * 2, 2, 0)
    targets = jnp.pad(teacher, ((0, 0), (0, 1))).reshape(ACTS)
    target = lax.dynamic_slice_in_dim(targets, tensor * 2, 2, 0)
    chosen = (target[:, None] == jnp.arange(BINS, dtype=jnp.int32)).astype(jnp.float32)

    shard = proj_w.T
    other = get(shard, dyh=1)
    first = yhi == 0
    both = jnp.concatenate([jnp.where(first, shard, other), jnp.where(first, other, shard)], axis=0)
    along = [both] + [get(both, dx=d) for d in (1, 2, 3)]
    columns = jnp.stack([jnp.stack([s, get(s, dc=1)]) for s in along]).reshape(512, V)

    own = patches.reshape(64, V)
    rows = lax.all_to_all(
        jnp.broadcast_to(own[None], (8, 64, V)), "tensor", 0, 0, tiled=True
    ).reshape(ROWS, V)

    qkv_pieces = weight_pieces(jnp.concatenate([wq, wk, wv], axis=1))
    wo_pieces = weight_pieces(jnp.concatenate([wo, get(wo, dyl=1)], axis=0))

    columns, table, acts, gain, actions_own, chosen = lax.optimization_barrier(
        (columns, table, acts, gain, actions_own, chosen)
    )
    embedded = lax.dot_general(
        rows, columns, (((1,), (1,)), ((), ())), preferred_element_type=jnp.float32
    ).astype(jnp.bfloat16)
    pair = (embedded, get(embedded, dyl=1))
    up = tuple(get(e, dz=1) for e in pair)
    down = tuple(get(e, dz=3) for e in pair)
    far = (get(up[0], dz=1), get(down[1], dz=3))
    blocks = [r[i] for i in range(2) for r in (pair, up, far, down)]

    qkv, embedded_own = project(table, gain, acts, blocks, qkv_pieces)
    mixed = attend(table, qkv)
    product, act_product = expand(table, mixed, get(mixed[1], dyl=1), wo_pieces)

    act_parts = jnp.transpose(act_product.reshape(NB, 4, 2, 256), (1, 2, 0, 3)).reshape(4, 2, D)
    act_parts = lax.all_to_all(
        act_parts, "tensor", 0, 0, tiled=True, axis_index_groups=[[0, 1, 2, 3], [4, 5, 6, 7]]
    )
    act_update = jnp.sum(act_parts.astype(jnp.float32), axis=0)
    acted = actions_own.astype(jnp.float32) + act_update
    final = normalize(acted, final_gain).astype(jnp.bfloat16)
    logits = jnp.dot(final, head_w, preferred_element_type=jnp.float32)
    picked = jnp.sum(logits * chosen, axis=-1)
    loss_own = jax.nn.logsumexp(logits, axis=-1) - picked
    loss = lax.all_to_all(jnp.broadcast_to(loss_own[None], (8, 2)), "tensor", 0, 0, tiled=True)
    loss = loss.reshape(FRAMES, SLOTS)[:, :ADIM]

    update = product[0].astype(jnp.float32)
    for b in range(1, 4):
        update = update + get(product[b], dz=-b).astype(jnp.float32)
    hidden = (embedded_own.astype(jnp.float32) + update).astype(jnp.bfloat16)
    hidden = jnp.transpose(hidden, (1, 0, 2)).reshape(FRAMES, 32, D)
    return (hidden, loss)


def solution(mesh):
    return jax.shard_map(
        on_device,
        mesh=mesh,
        in_specs=(
            P(("dp", "section"), "tensor", None),
            P(("dp", "section"), None),
            P(None, ("dp", "tensor", "section")),
            P(),
            P(("dp", "section"), "tensor"),
            P(("dp", "section"), "tensor"),
            P(("dp", "section"), "tensor"),
            P("tensor", ("dp", "section")),
            P(),
            P(),
            P(),
            P(),
        ),
        out_specs=(P(("dp", "section"), "tensor", None), P(("dp", "section"), None)),
        check_vma=False,
    )
```

```python
import math

import jax
import jax.numpy as jnp
import numpy as np
from jax import lax
from jax.experimental import pallas as pl
from jax.experimental.pallas import tpu as pltpu
from jax.sharding import PartitionSpec as P


D = 4096
HD = 128
V = 1152
P_SIZE = 256
BINS = 256
ADIM = 7
SLOTS = 8
FRAMES = 2
ROWS = FRAMES * P_SIZE
ACTS = FRAMES * SLOTS
HEADS = 4
NB = 16

eps = 1e-05


AXES = ("dp", "tensor", "section")
IDS = np.arange(128).reshape(4, 2, 2, 4, 2)
VMEM = pl.BlockSpec(memory_space=pltpu.VMEM)
SMEM = pl.BlockSpec(memory_space=pltpu.SMEM)
ANY = pl.BlockSpec(memory_space=pl.ANY)
LIMIT = pltpu.CompilerParams(vmem_limit_bytes=56 * 1024 * 1024)


def get(s, dx=0, dc=0, dyl=0, dz=0, dyh=0):
    pairs = []
    for x, c, yl, z, yh in np.ndindex(IDS.shape):
        source = IDS[(x + dx) % 4, c ^ dc, yl ^ dyl, (z + dz) % 4, yh ^ dyh]
        pairs.append((int(source), int(IDS[x, c, yl, z, yh])))
    return lax.ppermute(s, AXES, pairs)


def place():
    dp, tensor = lax.axis_index("dp"), lax.axis_index("tensor")
    return dp // 2, dp % 2, tensor // 4, tensor % 4, lax.axis_index("section")


def block_of(p):
    x, core, _, _, yhi = place()
    return (x + p // 4) % 4 * 4 + (core + p // 2) % 2 * 2 + (yhi + p) % 2


def weight_pieces(shard):
    near = (shard, get(shard, dyh=1))
    ahead = tuple(get(s, dx=1) for s in near)
    behind = tuple(get(s, dx=3) for s in near)
    across = (get(ahead[0], dx=1), get(behind[1], dx=3))
    pieces = []
    for ring in (near, ahead, across, behind):
        pieces += list(ring)
        pieces += [get(s, dc=1) for s in ring]
    return pieces


def normalize(rows, gain):
    rows = rows.astype(jnp.float32)
    factor = lax.rsqrt(jnp.mean(rows * rows, axis=-1, keepdims=True) + eps)
    return rows * factor * gain.astype(jnp.float32)


def join_kernel(q_ref, k_ref, v_ref, out_ref):
    width = q_ref.shape[1]
    for n, ref in enumerate((q_ref, k_ref, v_ref)):
        out_ref[:, n * width : (n + 1) * width] = ref[...]


def join(q, k, v):
    return pl.pallas_call(
        join_kernel,
        in_specs=[VMEM] * 3,
        out_specs=VMEM,
        out_shape=jax.ShapeDtypeStruct((q.shape[0], 3 * q.shape[1]), jnp.bfloat16),
        name="join",
    )(q, k, v)


def prepare_kernel(tokens_ref, start_ref, rows_ref, gain_ref, acts_ref, actions_ref, gains_ref):
    tokens = tokens_ref[...]
    picks = jnp.where(tokens == lax.broadcasted_iota(jnp.int32, (ACTS, BINS), 1), 1.0, 0.0)
    looked = jnp.dot(
        picks.astype(jnp.bfloat16), rows_ref[...], preferred_element_type=jnp.float32
    )
    actions = jnp.where(tokens < 0, start_ref[...].astype(jnp.float32), looked)
    actions_ref[...] = actions
    gain = gain_ref[...].astype(jnp.float32)
    factor = lax.rsqrt(jnp.sum(actions * actions, axis=-1, keepdims=True) * (1.0 / D) + eps)
    normed = (actions * factor * gain).astype(jnp.bfloat16)
    for nb in range(NB):
        acts_ref[nb] = normed[:, nb * 256 : (nb + 1) * 256]
        gains_ref[nb] = gain[:, nb * 256 : (nb + 1) * 256]


def prepare(teacher, start_row, action_table, norm_gain):
    tokens = jnp.pad(teacher, ((0, 0), (1, 0)), constant_values=-1).reshape(ACTS, 1)
    return pl.pallas_call(
        prepare_kernel,
        in_specs=[VMEM] * 4,
        out_specs=[VMEM] * 3,
        out_shape=[
            jax.ShapeDtypeStruct((NB, ACTS, 256), jnp.bfloat16),
            jax.ShapeDtypeStruct((ACTS, D), jnp.float32),
            jax.ShapeDtypeStruct((NB, 1, 256), jnp.float32),
        ],
        compiler_params=LIMIT,
        name="prepare",
    )(tokens, start_row.reshape(1, D), action_table, norm_gain.reshape(1, D))


def finish_kernel(loss_ref, emb_ref, *refs):
    parts, (out_ref, losses_ref) = refs[:4], refs[4:]
    for r in range(ACTS):
        if r % SLOTS < ADIM:
            losses_ref[r // SLOTS, r % SLOTS] = loss_ref[r // 2, r % 2]
    for nb in range(NB):
        total = emb_ref[nb].astype(jnp.float32)
        update = parts[0][nb].astype(jnp.float32) + parts[1][nb].astype(jnp.float32)
        update = update + parts[2][nb].astype(jnp.float32) + parts[3][nb].astype(jnp.float32)
        total = (total + update).astype(jnp.bfloat16)
        for f in range(FRAMES):
            out_ref[f, :, nb * 256 : (nb + 1) * 256] = total[f * 32 : (f + 1) * 32]


def finish(losses, embedded, parts):
    return pl.pallas_call(
        finish_kernel,
        in_specs=[SMEM] + [VMEM] * 5,
        out_specs=[VMEM, SMEM],
        out_shape=[
            jax.ShapeDtypeStruct((FRAMES, 32, D), jnp.bfloat16),
            jax.ShapeDtypeStruct((FRAMES, ADIM), jnp.float32),
        ],
        compiler_params=LIMIT,
        name="finish",
    )(losses, embedded, *parts)


def embed_kernel(rows_ref, *refs):
    pieces, (out_ref, columns_ref) = refs[:8], refs[8:]
    yhi = lax.axis_index("section")
    for p in range(8):
        for h in range(2):
            to = pl.ds(pl.multiple_of(p * 64 + (yhi + h) % 2 * 32, 32), 32)
            columns_ref[to, :] = pieces[p][h * 32 : (h + 1) * 32, :]
    out_ref[...] = lax.dot_general(
        rows_ref[...],
        columns_ref[...],
        (((1,), (1,)), ((), ())),
        preferred_element_type=jnp.float32,
    ).astype(jnp.bfloat16)


def embed(rows, pieces):
    return pl.pallas_call(
        embed_kernel,
        in_specs=[VMEM] * 9,
        out_specs=VMEM,
        out_shape=jax.ShapeDtypeStruct((ROWS, 512), jnp.bfloat16),
        scratch_shapes=[pltpu.VMEM((512, V), jnp.bfloat16)],
        compiler_params=LIMIT,
        name="embed",
    )(rows, *pieces)


def project_kernel(gain_ref, act_ref, *refs):
    x, core, own_ylo, z, _ = place()
    blocks, pieces = refs[:8], refs[8:24]
    out_ref, emb_ref, all_ref, normed_ref, sems = refs[24:]
    step = 32
    low = lax.broadcasted_iota(jnp.int32, (step, 128), 1) < 64

    def placed(rows, store):
        for ylo in range(2):
            for pair in range(2):
                for m in range(4):
                    cols = slice(m * 128, (m + 1) * 128)
                    a = all_ref[ylo * 4 + pair * 2, rows, cols].astype(jnp.float32)
                    b = all_ref[ylo * 4 + pair * 2 + 1, rows, cols].astype(jnp.float32)
                    at = slice(pair * 128, (pair + 1) * 128)
                    even = jnp.where(low, a, pltpu.roll(b, 64, 1))
                    odd = jnp.where(low, pltpu.roll(a, 64, 1), b)
                    at_x = (x + m) % 4 * 4 + ylo
                    store(at_x + core * 2, at, even)
                    store(at_x + (1 - core) * 2, at, odd)

    def chunk(i, carry):
        rows = pl.ds(pl.multiple_of(i * step, step), step)
        totals = [jnp.zeros((step, 128), jnp.float32) for _ in range(4)]
        for t in range(8):
            for m in range(4):
                v = all_ref[t, rows, m * 128 : (m + 1) * 128].astype(jnp.float32)
                totals[m] = totals[m] + v * v
        total = (totals[0] + totals[1]) + (totals[2] + totals[3])
        mean = jnp.sum(total, axis=1, keepdims=True) * (1.0 / D)
        factor = jnp.broadcast_to(lax.rsqrt(mean + eps), (step, 128))

        def store(nb, at, v):
            normed_ref[nb, rows, at] = (v * factor * gain_ref[nb, :, at]).astype(jnp.bfloat16)

        placed(rows, store)
        return carry

    def own_chunk(i, carry):
        to = pl.ds(pl.multiple_of(i * step, step), step)

        def store(nb, at, v):
            emb_ref[nb, to, at] = v.astype(jnp.bfloat16)

        placed(pl.ds(pl.multiple_of((own_ylo * 4 + z) * 64 + i * step, step), step), store)
        return carry

    @pl.when(pl.program_id(0) == 0)
    def _():
        copies = [
            pltpu.make_async_copy(blocks[r], all_ref.at[(own_ylo + r // 4) % 2 * 4 + (z + r) % 4], sems.at[r])
            for r in range(8)
        ]
        for copy in copies:
            copy.start()
        normed_ref[:, ROWS : ROWS + ACTS, :] = act_ref[...]
        for copy in copies:
            copy.wait()
        lax.fori_loop(0, ROWS // step, chunk, 0)
        lax.fori_loop(0, 2, own_chunk, 0)

    acc = None
    for p in range(16):
        part = jnp.dot(
            normed_ref[block_of(p)], pieces[p][...], preferred_element_type=jnp.float32
        )
        acc = part if acc is None else acc + part
    out_ref[...] = acc.astype(jnp.bfloat16)


def project(gain, acts, blocks, pieces):
    width = pieces[0].shape[1]
    tile = 512
    return pl.pallas_call(
        project_kernel,
        grid=(width // tile,),
        in_specs=[VMEM, VMEM]
        + [ANY] * 8
        + [pl.BlockSpec((256, tile), lambda n: (0, n))] * 16,
        out_specs=[
            pl.BlockSpec((ROWS + ACTS, tile), lambda n: (0, n)),
            pl.BlockSpec((NB, 64, 256), lambda n: (0, 0, 0)),
        ],
        out_shape=[
            jax.ShapeDtypeStruct((ROWS + ACTS, width), jnp.bfloat16),
            jax.ShapeDtypeStruct((NB, 64, 256), jnp.bfloat16),
        ],
        scratch_shapes=[
            pltpu.VMEM((8, ROWS, 512), jnp.bfloat16),
            pltpu.VMEM((NB, ROWS + ACTS, 256), jnp.bfloat16),
            pltpu.SemaphoreType.DMA((8,)),
        ],
        compiler_params=LIMIT,
        name="project",
    )(gain, acts, *blocks, *pieces)


def attend_kernel(qkv_ref, own_ref, other_ref, out_ref):
    own_ylo = place()[2]
    inv_root = 1.0 / math.sqrt(HD)
    width = HEADS * HD
    half = P_SIZE // 2
    causal = [
        lax.broadcasted_iota(jnp.int32, (half, n), 0) + (n - half)
        >= lax.broadcasted_iota(jnp.int32, (half, n), 1)
        for n in (half, P_SIZE)
    ]
    row_frame = lax.broadcasted_iota(jnp.int32, (ACTS, P_SIZE), 0) // SLOTS
    i = lax.broadcasted_iota(jnp.int32, (ACTS, ACTS), 0)
    j = lax.broadcasted_iota(jnp.int32, (ACTS, ACTS), 1)
    seen = (i // SLOTS == j // SLOTS) & (j <= i)

    def patch_rows(frame, start):
        return jnp.concatenate(
            [
                qkv_ref[t * 64 + frame * 32 : t * 64 + frame * 32 + 32, start : start + HD]
                for t in range(8)
            ],
            axis=0,
        )

    def scores(a, b):
        s = lax.dot_general(a, b, (((1,), (1,)), ((), ())), preferred_element_type=jnp.float32)
        return s * inv_root

    for h in range(HEADS):
        at = h * HD
        keys = [patch_rows(f, width + at) for f in range(FRAMES)]
        values = [patch_rows(f, 2 * width + at) for f in range(FRAMES)]
        for f in range(FRAMES):
            queries = patch_rows(f, at)
            for i_half, n in enumerate((half, P_SIZE)):
                q = queries[i_half * half : (i_half + 1) * half]
                s = jnp.where(causal[i_half], scores(q, keys[f][:n]), -1e30)
                e = jnp.exp(s - jnp.max(s, axis=-1, keepdims=True))
                total = jnp.sum(e, axis=-1, keepdims=True)
                o = jnp.dot(
                    e.astype(jnp.bfloat16), values[f][:n], preferred_element_type=jnp.float32
                )
                o = (o * (1.0 / total)).astype(jnp.bfloat16)
                side = (own_ylo + i_half) % 2
                for t in range(4):
                    row = t * 64 + f * 32
                    out_ref[side, row : row + 32, at : at + HD] = o[t * 32 : (t + 1) * 32]
        rows = slice(ROWS, ROWS + ACTS)
        qa = qkv_ref[rows, at : at + HD]
        ka = qkv_ref[rows, width + at : width + at + HD]
        va = qkv_ref[rows, 2 * width + at : 2 * width + at + HD]
        parts = [jnp.where(row_frame == f, scores(qa, keys[f]), -1e30) for f in range(FRAMES)]
        own = jnp.where(seen, scores(qa, ka), -1e30)
        top = jnp.max(own, axis=-1, keepdims=True)
        for s in parts:
            top = jnp.maximum(top, jnp.max(s, axis=-1, keepdims=True))
        parts = [jnp.exp(s - top) for s in parts]
        own = jnp.exp(own - top)
        total = jnp.sum(own, axis=-1, keepdims=True)
        for e in parts:
            total = total + jnp.sum(e, axis=-1, keepdims=True)
        mixed = jnp.dot(own.astype(jnp.bfloat16), va, preferred_element_type=jnp.float32)
        for e, v in zip(parts, values):
            mixed = mixed + jnp.dot(
                e.astype(jnp.bfloat16), v, preferred_element_type=jnp.float32
            )
        mixed = mixed * (1.0 / total)
        for f in range(FRAMES):
            out_ref[(own_ylo + f) % 2, 256:264, at : at + HD] = mixed[
                f * SLOTS : (f + 1) * SLOTS
            ].astype(jnp.bfloat16)
    own_ref[...] = out_ref[0]
    other_ref[...] = out_ref[1]


def attend(qkv):
    shape = (264, HEADS * HD)
    return pl.pallas_call(
        attend_kernel,
        in_specs=[VMEM],
        out_specs=[VMEM, VMEM],
        out_shape=[jax.ShapeDtypeStruct(shape, jnp.bfloat16)] * 2,
        scratch_shapes=[pltpu.VMEM((2, *shape), jnp.bfloat16)],
        compiler_params=LIMIT,
        name="attend",
    )(qkv)


def expand_kernel(own_ref, other_ref, *refs):
    pieces, outs, (act_ref, acc_ref) = refs[:16], refs[16:20], refs[20:]
    own, other = own_ref[...], other_ref[...]
    for p in range(16):
        acc = jnp.dot(own, pieces[p][:512], preferred_element_type=jnp.float32)
        acc = acc + jnp.dot(other, pieces[p][512:], preferred_element_type=jnp.float32)
        nb = block_of(p)
        acc_ref[p % 2] = acc[:256].astype(jnp.bfloat16)
        for t in range(4):
            act_ref[t, nb] = acc[256 + 2 * t : 258 + 2 * t].astype(jnp.bfloat16)
        for b in range(4):
            rows = pl.ds(pl.multiple_of((place()[3] + b) % 4 * 64, 64), 64)
            outs[b][nb] = acc_ref[p % 2, rows]


def expand(mixed, other, pieces):
    return pl.pallas_call(
        expand_kernel,
        in_specs=[VMEM] * 18,
        out_specs=[VMEM] * 5,
        out_shape=[jax.ShapeDtypeStruct((NB, 64, 256), jnp.bfloat16)] * 4
        + [jax.ShapeDtypeStruct((4, NB, 2, 256), jnp.bfloat16)],
        scratch_shapes=[pltpu.VMEM((2, 256, 256), jnp.bfloat16)],
        compiler_params=LIMIT,
        name="expand",
    )(mixed, other, *pieces)


def on_device(
    patches, teacher, proj_w, norm_gain, wq, wk, wv, wo, start_row, action_table, final_gain, head_w
):
    tensor = lax.axis_index("tensor")

    shard = proj_w.T
    both = jnp.concatenate([shard, get(shard, dyh=1)], axis=0)
    along = [both] + [get(both, dx=d) for d in (1, 2, 3)]
    columns = [s for near in along for s in (near, get(near, dc=1))]

    own = patches.reshape(64, V)
    rows = lax.all_to_all(
        jnp.broadcast_to(own[None], (8, 64, V)), "tensor", 0, 0, tiled=True
    ).reshape(ROWS, V)

    qkv_pieces = weight_pieces(join(wq, wk, wv))
    wo_pieces = weight_pieces(jnp.concatenate([wo, get(wo, dyl=1)], axis=0))

    acts, actions, gain = prepare(teacher, start_row, action_table, norm_gain)
    rows, acts, gain = lax.optimization_barrier((rows, acts, gain))
    embedded = embed(rows, columns)
    pair = (embedded, get(embedded, dyl=1))
    up = tuple(get(e, dz=1) for e in pair)
    down = tuple(get(e, dz=3) for e in pair)
    far = (get(up[0], dz=1), get(down[1], dz=3))
    blocks = [r[i] for i in range(2) for r in (pair, up, far, down)]

    qkv, embedded_own = project(gain, acts, blocks, qkv_pieces)
    mixed, other = attend(qkv)
    *product, act_product = expand(mixed, get(other, dyl=1), wo_pieces)

    act_parts = act_product
    act_parts = lax.all_to_all(
        act_parts, "tensor", 0, 0, tiled=True, axis_index_groups=[[0, 1, 2, 3], [4, 5, 6, 7]]
    )
    act_update = jnp.sum(act_parts.astype(jnp.float32), axis=0)
    act_update = jnp.transpose(act_update, (1, 0, 2)).reshape(2, D)
    acted = lax.dynamic_slice_in_dim(actions, tensor * 2, 2, 0) + act_update
    final = normalize(acted, final_gain).astype(jnp.bfloat16)
    logits = jnp.dot(final, head_w, preferred_element_type=jnp.float32)
    targets = jnp.pad(teacher, ((0, 0), (0, 1))).reshape(ACTS)
    target = lax.dynamic_slice_in_dim(targets, tensor * 2, 2, 0)
    chosen = (target[:, None] == jnp.arange(BINS, dtype=jnp.int32)).astype(jnp.float32)
    picked = jnp.sum(logits * chosen, axis=-1)
    loss_own = jax.nn.logsumexp(logits, axis=-1) - picked
    loss = lax.all_to_all(jnp.broadcast_to(loss_own[None], (8, 2)), "tensor", 0, 0, tiled=True)
    parts = [product[0]] + [get(product[b], dz=-b) for b in range(1, 4)]
    return tuple(finish(loss, embedded_own, parts))


def solution(mesh):
    return jax.shard_map(
        on_device,
        mesh=mesh,
        in_specs=(
            P(("dp", "section"), "tensor", None),
            P(("dp", "section"), None),
            P(None, ("dp", "tensor", "section")),
            P(),
            P(("dp", "section"), "tensor"),
            P(("dp", "section"), "tensor"),
            P(("dp", "section"), "tensor"),
            P("tensor", ("dp", "section")),
            P(),
            P(),
            P(),
            P(),
        ),
        out_specs=(P(("dp", "section"), "tensor", None), P(("dp", "section"), None)),
        check_vma=False,
    )
```

```python
import math

import jax
import jax.numpy as jnp
import numpy as np
from jax import lax
from jax.experimental import pallas as pl
from jax.experimental.pallas import tpu as pltpu
from jax.sharding import PartitionSpec as P


D = 4096
HD = 128
V = 1152
P_SIZE = 256
BINS = 256
ADIM = 7
SLOTS = 8
FRAMES = 2
ROWS = FRAMES * P_SIZE
ACTS = FRAMES * SLOTS
HEADS = 4
NB = 16

eps = 1e-05


AXES = ("dp", "tensor", "section")
IDS = np.arange(128).reshape(4, 2, 2, 4, 2)
VMEM = pl.BlockSpec(memory_space=pltpu.VMEM)
SMEM = pl.BlockSpec(memory_space=pltpu.SMEM)
ANY = pl.BlockSpec(memory_space=pl.ANY)
LIMIT = pltpu.CompilerParams(vmem_limit_bytes=56 * 1024 * 1024)


def get(s, dx=0, dc=0, dyl=0, dz=0, dyh=0):
    pairs = []
    for x, c, yl, z, yh in np.ndindex(IDS.shape):
        source = IDS[(x + dx) % 4, c ^ dc, yl ^ dyl, (z + dz) % 4, yh ^ dyh]
        pairs.append((int(source), int(IDS[x, c, yl, z, yh])))
    return lax.ppermute(s, AXES, pairs)


def place():
    dp, tensor = lax.axis_index("dp"), lax.axis_index("tensor")
    return dp // 2, dp % 2, tensor // 4, tensor % 4, lax.axis_index("section")


def block_of(p):
    x, core, _, _, yhi = place()
    return (x + p // 4) % 4 * 4 + (core + p // 2) % 2 * 2 + (yhi + p) % 2


def weight_pieces(shard):
    near = (shard, get(shard, dyh=1))
    ahead = tuple(get(s, dx=1) for s in near)
    behind = tuple(get(s, dx=3) for s in near)
    across = (get(ahead[0], dx=1), get(behind[1], dx=3))
    pieces = []
    for ring in (near, ahead, across, behind):
        pieces += list(ring)
        pieces += [get(s, dc=1) for s in ring]
    return pieces


def normalize(rows, gain):
    rows = rows.astype(jnp.float32)
    factor = lax.rsqrt(jnp.mean(rows * rows, axis=-1, keepdims=True) + eps)
    return rows * factor * gain.astype(jnp.float32)


def join_kernel(q_ref, k_ref, v_ref, out_ref):
    width = q_ref.shape[1]
    for n, ref in enumerate((q_ref, k_ref, v_ref)):
        out_ref[:, n * width : (n + 1) * width] = ref[...]


def join(q, k, v):
    return pl.pallas_call(
        join_kernel,
        in_specs=[VMEM] * 3,
        out_specs=VMEM,
        out_shape=jax.ShapeDtypeStruct((q.shape[0], 3 * q.shape[1]), jnp.bfloat16),
        name="join",
    )(q, k, v)


def prepare_kernel(tokens_ref, start_ref, rows_ref, gain_ref, acts_ref, actions_ref, gains_ref):
    tokens = tokens_ref[...]
    picks = jnp.where(tokens == lax.broadcasted_iota(jnp.int32, (ACTS, BINS), 1), 1.0, 0.0)
    looked = jnp.dot(
        picks.astype(jnp.bfloat16), rows_ref[...], preferred_element_type=jnp.float32
    )
    actions = jnp.where(tokens < 0, start_ref[...].astype(jnp.float32), looked)
    actions_ref[...] = actions
    gain = gain_ref[...].astype(jnp.float32)
    factor = lax.rsqrt(jnp.sum(actions * actions, axis=-1, keepdims=True) * (1.0 / D) + eps)
    normed = (actions * factor * gain).astype(jnp.bfloat16)
    for nb in range(NB):
        acts_ref[nb] = normed[:, nb * 256 : (nb + 1) * 256]
        gains_ref[nb] = gain[:, nb * 256 : (nb + 1) * 256]


def prepare(teacher, start_row, action_table, norm_gain):
    tokens = jnp.pad(teacher, ((0, 0), (1, 0)), constant_values=-1).reshape(ACTS, 1)
    return pl.pallas_call(
        prepare_kernel,
        in_specs=[VMEM] * 4,
        out_specs=[VMEM] * 3,
        out_shape=[
            jax.ShapeDtypeStruct((NB, ACTS, 256), jnp.bfloat16),
            jax.ShapeDtypeStruct((ACTS, D), jnp.float32),
            jax.ShapeDtypeStruct((NB, 1, 256), jnp.float32),
        ],
        compiler_params=LIMIT,
        name="prepare",
    )(tokens, start_row.reshape(1, D), action_table, norm_gain.reshape(1, D))


def finish_kernel(loss_ref, emb_ref, *refs):
    parts, (out_ref, losses_ref) = refs[:4], refs[4:]
    for r in range(ACTS):
        if r % SLOTS < ADIM:
            losses_ref[r // SLOTS, r % SLOTS] = loss_ref[r // 2, r % 2]
    for nb in range(NB):
        total = emb_ref[nb].astype(jnp.float32)
        update = parts[0][nb].astype(jnp.float32) + parts[1][nb].astype(jnp.float32)
        update = update + parts[2][nb].astype(jnp.float32) + parts[3][nb].astype(jnp.float32)
        total = (total + update).astype(jnp.bfloat16)
        for f in range(FRAMES):
            out_ref[f, :, nb * 256 : (nb + 1) * 256] = total[f * 32 : (f + 1) * 32]


def finish(losses, embedded, parts):
    return pl.pallas_call(
        finish_kernel,
        in_specs=[SMEM] + [VMEM] * 5,
        out_specs=[VMEM, SMEM],
        out_shape=[
            jax.ShapeDtypeStruct((FRAMES, 32, D), jnp.bfloat16),
            jax.ShapeDtypeStruct((FRAMES, ADIM), jnp.float32),
        ],
        compiler_params=LIMIT,
        name="finish",
    )(losses, embedded, *parts)


def embed_kernel(rows_ref, *refs):
    pieces, (out_ref, columns_ref) = refs[:8], refs[8:]
    yhi = lax.axis_index("section")
    for p in range(8):
        for h in range(2):
            to = pl.ds(pl.multiple_of(p * 64 + (yhi + h) % 2 * 32, 32), 32)
            columns_ref[to, :] = pieces[p][h * 32 : (h + 1) * 32, :]
    out_ref[...] = lax.dot_general(
        rows_ref[...],
        columns_ref[...],
        (((1,), (1,)), ((), ())),
        preferred_element_type=jnp.float32,
    ).astype(jnp.bfloat16)


def embed(rows, pieces):
    return pl.pallas_call(
        embed_kernel,
        in_specs=[VMEM] * 9,
        out_specs=VMEM,
        out_shape=jax.ShapeDtypeStruct((ROWS, 512), jnp.bfloat16),
        scratch_shapes=[pltpu.VMEM((512, V), jnp.bfloat16)],
        compiler_params=LIMIT,
        name="embed",
    )(rows, *pieces)


def project_kernel(gain_ref, act_ref, *refs):
    x, core, own_ylo, z, _ = place()
    blocks, pieces = refs[:8], refs[8:24]
    out_ref, emb_ref, all_ref, normed_ref, sems = refs[24:]
    step = 32
    low = lax.broadcasted_iota(jnp.int32, (step, 128), 1) < 64

    def placed(rows, store):
        for ylo in range(2):
            for pair in range(2):
                for m in range(4):
                    cols = slice(m * 128, (m + 1) * 128)
                    a = all_ref[ylo * 4 + pair * 2, rows, cols].astype(jnp.float32)
                    b = all_ref[ylo * 4 + pair * 2 + 1, rows, cols].astype(jnp.float32)
                    at = slice(pair * 128, (pair + 1) * 128)
                    even = jnp.where(low, a, pltpu.roll(b, 64, 1))
                    odd = jnp.where(low, pltpu.roll(a, 64, 1), b)
                    at_x = (x + m) % 4 * 4 + ylo
                    store(at_x + core * 2, at, even)
                    store(at_x + (1 - core) * 2, at, odd)

    def chunk(i, carry):
        rows = pl.ds(pl.multiple_of(i * step, step), step)
        totals = [jnp.zeros((step, 128), jnp.float32) for _ in range(4)]
        for t in range(8):
            for m in range(4):
                v = all_ref[t, rows, m * 128 : (m + 1) * 128].astype(jnp.float32)
                totals[m] = totals[m] + v * v
        total = (totals[0] + totals[1]) + (totals[2] + totals[3])
        mean = jnp.sum(total, axis=1, keepdims=True) * (1.0 / D)
        factor = jnp.broadcast_to(lax.rsqrt(mean + eps), (step, 128))

        def store(nb, at, v):
            normed_ref[nb, rows, at] = (v * factor * gain_ref[nb, :, at]).astype(jnp.bfloat16)

        placed(rows, store)
        return carry

    def own_chunk(i, carry):
        to = pl.ds(pl.multiple_of(i * step, step), step)

        def store(nb, at, v):
            emb_ref[nb, to, at] = v.astype(jnp.bfloat16)

        placed(pl.ds(pl.multiple_of((own_ylo * 4 + z) * 64 + i * step, step), step), store)
        return carry

    @pl.when(pl.program_id(0) == 0)
    def _():
        copies = [
            pltpu.make_async_copy(blocks[r], all_ref.at[(own_ylo + r // 4) % 2 * 4 + (z + r) % 4], sems.at[r])
            for r in range(8)
        ]
        for copy in copies:
            copy.start()
        normed_ref[:, ROWS : ROWS + ACTS, :] = act_ref[...]
        for copy in copies:
            copy.wait()
        lax.fori_loop(0, ROWS // step, chunk, 0)
        lax.fori_loop(0, 2, own_chunk, 0)

    acc = None
    for p in range(0, 16, 4):
        part = jnp.dot(
            jnp.concatenate([normed_ref[block_of(p + i)] for i in range(4)], axis=1),
            jnp.concatenate([pieces[p + i][...] for i in range(4)], axis=0),
            preferred_element_type=jnp.float32,
        )
        acc = part if acc is None else acc + part
    out_ref[...] = acc.astype(jnp.bfloat16)


def project(gain, acts, blocks, pieces):
    width = pieces[0].shape[1]
    tile = 512
    return pl.pallas_call(
        project_kernel,
        grid=(width // tile,),
        in_specs=[VMEM, VMEM]
        + [ANY] * 8
        + [pl.BlockSpec((256, tile), lambda n: (0, n))] * 16,
        out_specs=[
            pl.BlockSpec((ROWS + ACTS, tile), lambda n: (0, n)),
            pl.BlockSpec((NB, 64, 256), lambda n: (0, 0, 0)),
        ],
        out_shape=[
            jax.ShapeDtypeStruct((ROWS + ACTS, width), jnp.bfloat16),
            jax.ShapeDtypeStruct((NB, 64, 256), jnp.bfloat16),
        ],
        scratch_shapes=[
            pltpu.VMEM((8, ROWS, 512), jnp.bfloat16),
            pltpu.VMEM((NB, ROWS + ACTS, 256), jnp.bfloat16),
            pltpu.SemaphoreType.DMA((8,)),
        ],
        compiler_params=LIMIT,
        name="project",
    )(gain, acts, *blocks, *pieces)


def attend_kernel(qkv_ref, own_ref, other_ref, out_ref):
    own_ylo = place()[2]
    inv_root = 1.0 / math.sqrt(HD)
    width = HEADS * HD
    half = P_SIZE // 2
    causal = [
        lax.broadcasted_iota(jnp.int32, (half, n), 0) + (n - half)
        >= lax.broadcasted_iota(jnp.int32, (half, n), 1)
        for n in (half, P_SIZE)
    ]
    row_frame = lax.broadcasted_iota(jnp.int32, (ACTS, P_SIZE), 0) // SLOTS
    i = lax.broadcasted_iota(jnp.int32, (ACTS, ACTS), 0)
    j = lax.broadcasted_iota(jnp.int32, (ACTS, ACTS), 1)
    seen = (i // SLOTS == j // SLOTS) & (j <= i)

    def patch_rows(frame, start):
        return jnp.concatenate(
            [
                qkv_ref[t * 64 + frame * 32 : t * 64 + frame * 32 + 32, start : start + HD]
                for t in range(8)
            ],
            axis=0,
        )

    def scores(a, b):
        s = lax.dot_general(a, b, (((1,), (1,)), ((), ())), preferred_element_type=jnp.float32)
        return s * inv_root

    for h in range(HEADS):
        at = h * HD
        keys = [patch_rows(f, width + at) for f in range(FRAMES)]
        values = [patch_rows(f, 2 * width + at) for f in range(FRAMES)]
        for f in range(FRAMES):
            queries = patch_rows(f, at)
            for i_half, n in enumerate((half, P_SIZE)):
                q = queries[i_half * half : (i_half + 1) * half]
                s = jnp.where(causal[i_half], scores(q, keys[f][:n]), -1e30)
                e = jnp.exp(s - jnp.max(s, axis=-1, keepdims=True))
                total = jnp.sum(e, axis=-1, keepdims=True)
                o = jnp.dot(
                    e.astype(jnp.bfloat16), values[f][:n], preferred_element_type=jnp.float32
                )
                o = (o * (1.0 / total)).astype(jnp.bfloat16)
                side = (own_ylo + i_half) % 2
                for t in range(4):
                    row = t * 64 + f * 32
                    out_ref[side, row : row + 32, at : at + HD] = o[t * 32 : (t + 1) * 32]
        rows = slice(ROWS, ROWS + ACTS)
        qa = qkv_ref[rows, at : at + HD]
        ka = qkv_ref[rows, width + at : width + at + HD]
        va = qkv_ref[rows, 2 * width + at : 2 * width + at + HD]
        parts = [jnp.where(row_frame == f, scores(qa, keys[f]), -1e30) for f in range(FRAMES)]
        own = jnp.where(seen, scores(qa, ka), -1e30)
        top = jnp.max(own, axis=-1, keepdims=True)
        for s in parts:
            top = jnp.maximum(top, jnp.max(s, axis=-1, keepdims=True))
        parts = [jnp.exp(s - top) for s in parts]
        own = jnp.exp(own - top)
        total = jnp.sum(own, axis=-1, keepdims=True)
        for e in parts:
            total = total + jnp.sum(e, axis=-1, keepdims=True)
        mixed = jnp.dot(own.astype(jnp.bfloat16), va, preferred_element_type=jnp.float32)
        for e, v in zip(parts, values):
            mixed = mixed + jnp.dot(
                e.astype(jnp.bfloat16), v, preferred_element_type=jnp.float32
            )
        mixed = mixed * (1.0 / total)
        for f in range(FRAMES):
            out_ref[(own_ylo + f) % 2, 256:264, at : at + HD] = mixed[
                f * SLOTS : (f + 1) * SLOTS
            ].astype(jnp.bfloat16)
    own_ref[...] = out_ref[0]
    other_ref[...] = out_ref[1]


def attend(qkv):
    shape = (264, HEADS * HD)
    return pl.pallas_call(
        attend_kernel,
        in_specs=[VMEM],
        out_specs=[VMEM, VMEM],
        out_shape=[jax.ShapeDtypeStruct(shape, jnp.bfloat16)] * 2,
        scratch_shapes=[pltpu.VMEM((2, *shape), jnp.bfloat16)],
        compiler_params=LIMIT,
        name="attend",
    )(qkv)


def expand_kernel(own_ref, other_ref, *refs):
    pieces, outs, (act_ref, acc_ref) = refs[:16], refs[16:20], refs[20:]
    mixed = jnp.concatenate([own_ref[...], other_ref[...]], axis=1)
    for p in range(16):
        acc = jnp.dot(mixed, pieces[p][...], preferred_element_type=jnp.float32)
        nb = block_of(p)
        acc_ref[p % 2] = acc[:256].astype(jnp.bfloat16)
        for t in range(4):
            act_ref[t, nb] = acc[256 + 2 * t : 258 + 2 * t].astype(jnp.bfloat16)
        for b in range(4):
            rows = pl.ds(pl.multiple_of((place()[3] + b) % 4 * 64, 64), 64)
            outs[b][nb] = acc_ref[p % 2, rows]


def expand(mixed, other, pieces):
    return pl.pallas_call(
        expand_kernel,
        in_specs=[VMEM] * 18,
        out_specs=[VMEM] * 5,
        out_shape=[jax.ShapeDtypeStruct((NB, 64, 256), jnp.bfloat16)] * 4
        + [jax.ShapeDtypeStruct((4, NB, 2, 256), jnp.bfloat16)],
        scratch_shapes=[pltpu.VMEM((2, 256, 256), jnp.bfloat16)],
        compiler_params=LIMIT,
        name="expand",
    )(mixed, other, *pieces)


def on_device(
    patches, teacher, proj_w, norm_gain, wq, wk, wv, wo, start_row, action_table, final_gain, head_w
):
    tensor = lax.axis_index("tensor")

    shard = proj_w.T
    both = jnp.concatenate([shard, get(shard, dyh=1)], axis=0)
    along = [both] + [get(both, dx=d) for d in (1, 2, 3)]
    columns = [s for near in along for s in (near, get(near, dc=1))]

    own = patches.reshape(64, V)
    rows = lax.all_to_all(
        jnp.broadcast_to(own[None], (8, 64, V)), "tensor", 0, 0, tiled=True
    ).reshape(ROWS, V)

    qkv_pieces = weight_pieces(join(wq, wk, wv))
    wo_pieces = weight_pieces(jnp.concatenate([wo, get(wo, dyl=1)], axis=0))

    acts, actions, gain = prepare(teacher, start_row, action_table, norm_gain)
    rows, acts, gain = lax.optimization_barrier((rows, acts, gain))
    embedded = embed(rows, columns)
    pair = (embedded, get(embedded, dyl=1))
    up = tuple(get(e, dz=1) for e in pair)
    down = tuple(get(e, dz=3) for e in pair)
    far = (get(up[0], dz=1), get(down[1], dz=3))
    blocks = [r[i] for i in range(2) for r in (pair, up, far, down)]

    qkv, embedded_own = project(gain, acts, blocks, qkv_pieces)
    mixed, other = attend(qkv)
    *product, act_product = expand(mixed, get(other, dyl=1), wo_pieces)

    act_parts = act_product
    act_parts = lax.all_to_all(
        act_parts, "tensor", 0, 0, tiled=True, axis_index_groups=[[0, 1, 2, 3], [4, 5, 6, 7]]
    )
    act_update = jnp.sum(act_parts.astype(jnp.float32), axis=0)
    act_update = jnp.transpose(act_update, (1, 0, 2)).reshape(2, D)
    acted = lax.dynamic_slice_in_dim(actions, tensor * 2, 2, 0) + act_update
    final = normalize(acted, final_gain).astype(jnp.bfloat16)
    logits = jnp.dot(final, head_w, preferred_element_type=jnp.float32)
    targets = jnp.pad(teacher, ((0, 0), (0, 1))).reshape(ACTS)
    target = lax.dynamic_slice_in_dim(targets, tensor * 2, 2, 0)
    chosen = (target[:, None] == jnp.arange(BINS, dtype=jnp.int32)).astype(jnp.float32)
    picked = jnp.sum(logits * chosen, axis=-1)
    loss_own = jax.nn.logsumexp(logits, axis=-1) - picked
    loss = lax.all_to_all(jnp.broadcast_to(loss_own[None], (8, 2)), "tensor", 0, 0, tiled=True)
    parts = [product[0]] + [get(product[b], dz=-b) for b in range(1, 4)]
    return tuple(finish(loss, embedded_own, parts))


def solution(mesh):
    return jax.shard_map(
        on_device,
        mesh=mesh,
        in_specs=(
            P(("dp", "section"), "tensor", None),
            P(("dp", "section"), None),
            P(None, ("dp", "tensor", "section")),
            P(),
            P(("dp", "section"), "tensor"),
            P(("dp", "section"), "tensor"),
            P(("dp", "section"), "tensor"),
            P("tensor", ("dp", "section")),
            P(),
            P(),
            P(),
            P(),
        ),
        out_specs=(P(("dp", "section"), "tensor", None), P(("dp", "section"), None)),
        check_vma=False,
    )
```

```python
import functools
import math

import jax
import jax.numpy as jnp
import numpy as np
from jax import lax
from jax.experimental import pallas as pl
from jax.experimental.pallas import tpu as pltpu
from jax.sharding import PartitionSpec as P


D = 4096
HD = 128
V = 1152
P_SIZE = 256
BINS = 256
ADIM = 7
SLOTS = 8
FRAMES = 2
ROWS = FRAMES * P_SIZE
ACTS = FRAMES * SLOTS
HEADS = 4
NB = 16

eps = 1e-05


AXES = ("dp", "tensor", "section")
IDS = np.arange(128).reshape(4, 2, 2, 4, 2)
VMEM = pl.BlockSpec(memory_space=pltpu.VMEM)
SMEM = pl.BlockSpec(memory_space=pltpu.SMEM)
ANY = pl.BlockSpec(memory_space=pl.ANY)
LIMIT = pltpu.CompilerParams(vmem_limit_bytes=56 * 1024 * 1024)


def get(s, dx=0, dc=0, dyl=0, dz=0, dyh=0):
    pairs = []
    for x, c, yl, z, yh in np.ndindex(IDS.shape):
        source = IDS[(x + dx) % 4, c ^ dc, yl ^ dyl, (z + dz) % 4, yh ^ dyh]
        pairs.append((int(source), int(IDS[x, c, yl, z, yh])))
    return lax.ppermute(s, AXES, pairs)


def place():
    dp, tensor = lax.axis_index("dp"), lax.axis_index("tensor")
    return dp // 2, dp % 2, tensor // 4, tensor % 4, lax.axis_index("section")


def block_of(p):
    x, core, _, _, yhi = place()
    return (x + p // 4) % 4 * 4 + (core + p // 2) % 2 * 2 + (yhi + p) % 2


def weight_pieces(shard):
    near = (shard, get(shard, dyh=1))
    ahead = tuple(get(s, dx=1) for s in near)
    behind = tuple(get(s, dx=3) for s in near)
    across = (get(ahead[0], dx=1), get(behind[1], dx=3))
    pieces = []
    for ring in (near, ahead, across, behind):
        pieces += list(ring)
        pieces += [get(s, dc=1) for s in ring]
    return pieces


def normalize(rows, gain):
    rows = rows.astype(jnp.float32)
    factor = lax.rsqrt(jnp.mean(rows * rows, axis=-1, keepdims=True) + eps)
    return rows * factor * gain.astype(jnp.float32)


def join_kernel(q_ref, k_ref, v_ref, out_ref):
    width = q_ref.shape[1]
    for n, ref in enumerate((q_ref, k_ref, v_ref)):
        out_ref[:, n * width : (n + 1) * width] = ref[...]


def join(q, k, v):
    return pl.pallas_call(
        join_kernel,
        in_specs=[VMEM] * 3,
        out_specs=VMEM,
        out_shape=jax.ShapeDtypeStruct((q.shape[0], 3 * q.shape[1]), jnp.bfloat16),
        name="join",
    )(q, k, v)


def prepare_kernel(tokens_ref, start_ref, rows_ref, gain_ref, acts_ref, actions_ref, gains_ref):
    tokens = tokens_ref[...]
    picks = jnp.where(tokens == lax.broadcasted_iota(jnp.int32, (ACTS, BINS), 1), 1.0, 0.0)
    looked = jnp.dot(
        picks.astype(jnp.bfloat16), rows_ref[...], preferred_element_type=jnp.float32
    )
    actions = jnp.where(tokens < 0, start_ref[...].astype(jnp.float32), looked)
    actions_ref[...] = actions
    gain = gain_ref[...].astype(jnp.float32)
    factor = lax.rsqrt(jnp.sum(actions * actions, axis=-1, keepdims=True) * (1.0 / D) + eps)
    normed = (actions * factor * gain).astype(jnp.bfloat16)
    for nb in range(NB):
        acts_ref[nb] = normed[:, nb * 256 : (nb + 1) * 256]
        gains_ref[nb] = gain[:, nb * 256 : (nb + 1) * 256]


def prepare(teacher, start_row, action_table, norm_gain):
    tokens = jnp.pad(teacher, ((0, 0), (1, 0)), constant_values=-1).reshape(ACTS, 1)
    return pl.pallas_call(
        prepare_kernel,
        in_specs=[VMEM] * 4,
        out_specs=[VMEM] * 3,
        out_shape=[
            jax.ShapeDtypeStruct((NB, ACTS, 256), jnp.bfloat16),
            jax.ShapeDtypeStruct((ACTS, D), jnp.float32),
            jax.ShapeDtypeStruct((NB, 1, 256), jnp.float32),
        ],
        compiler_params=LIMIT,
        name="prepare",
    )(tokens, start_row.reshape(1, D), action_table, norm_gain.reshape(1, D))


def finish_kernel(loss_ref, other_ref, emb_ref, *refs):
    parts, (out_ref, losses_ref) = refs[:8], refs[8:]
    own_ylo = place()[2]
    for a in range(ADIM):
        losses_ref[own_ylo, a] = loss_ref[a]
        losses_ref[1 - own_ylo, a] = other_ref[a]
    for p in range(NB):
        nb = block_of(p)
        of = [part[p % 8].astype(jnp.float32) for part in parts[p // 8 * 4 : p // 8 * 4 + 4]]
        update = (of[0] + of[1]) + (of[2] + of[3])
        total = (emb_ref[nb].astype(jnp.float32) + update).astype(jnp.bfloat16)
        cols = pl.ds(pl.multiple_of(nb * 256, 256), 256)
        for f in range(FRAMES):
            out_ref[f, :, cols] = total[f * 32 : (f + 1) * 32]


def finish(loss, other, embedded, parts):
    return pl.pallas_call(
        finish_kernel,
        in_specs=[SMEM] * 2 + [VMEM] * 9,
        out_specs=[VMEM, SMEM],
        out_shape=[
            jax.ShapeDtypeStruct((FRAMES, 32, D), jnp.bfloat16),
            jax.ShapeDtypeStruct((FRAMES, ADIM), jnp.float32),
        ],
        compiler_params=LIMIT,
        name="finish",
    )(loss, other, embedded, *parts)


def embed_kernel(rows_ref, *refs):
    pieces, (out_ref, columns_ref) = refs[:8], refs[8:]
    yhi = lax.axis_index("section")
    for p in range(8):
        for h in range(2):
            to = pl.ds(pl.multiple_of(p * 64 + (yhi + h) % 2 * 32, 32), 32)
            columns_ref[to, :] = pieces[p][h * 32 : (h + 1) * 32, :]
    out_ref[...] = lax.dot_general(
        rows_ref[...],
        columns_ref[...],
        (((1,), (1,)), ((), ())),
        preferred_element_type=jnp.float32,
    ).astype(jnp.bfloat16)


def embed(rows, pieces):
    return pl.pallas_call(
        embed_kernel,
        in_specs=[VMEM] * 9,
        out_specs=VMEM,
        out_shape=jax.ShapeDtypeStruct((ROWS, 512), jnp.bfloat16),
        scratch_shapes=[pltpu.VMEM((512, V), jnp.bfloat16)],
        compiler_params=LIMIT,
        name="embed",
    )(rows, *pieces)


def project_kernel(gain_ref, act_ref, *refs):
    x, core, own_ylo, z, _ = place()
    blocks, pieces = refs[:8], refs[8:24]
    out_ref, emb_ref, all_ref, normed_ref, sems = refs[24:]
    step = 32
    low = lax.broadcasted_iota(jnp.int32, (step, 128), 1) < 64

    def placed(rows, store):
        for ylo in range(2):
            for pair in range(2):
                for m in range(4):
                    cols = slice(m * 128, (m + 1) * 128)
                    a = all_ref[ylo * 4 + pair * 2, rows, cols].astype(jnp.float32)
                    b = all_ref[ylo * 4 + pair * 2 + 1, rows, cols].astype(jnp.float32)
                    at = slice(pair * 128, (pair + 1) * 128)
                    even = jnp.where(low, a, pltpu.roll(b, 64, 1))
                    odd = jnp.where(low, pltpu.roll(a, 64, 1), b)
                    at_x = (x + m) % 4 * 4 + ylo
                    store(at_x + core * 2, at, even)
                    store(at_x + (1 - core) * 2, at, odd)

    def chunk(i, carry):
        rows = pl.ds(pl.multiple_of(i * step, step), step)
        totals = [jnp.zeros((step, 128), jnp.float32) for _ in range(4)]
        for t in range(8):
            for m in range(4):
                v = all_ref[t, rows, m * 128 : (m + 1) * 128].astype(jnp.float32)
                totals[m] = totals[m] + v * v
        total = (totals[0] + totals[1]) + (totals[2] + totals[3])
        mean = jnp.sum(total, axis=1, keepdims=True) * (1.0 / D)
        factor = jnp.broadcast_to(lax.rsqrt(mean + eps), (step, 128))

        def store(nb, at, v):
            normed_ref[nb, rows, at] = (v * factor * gain_ref[nb, :, at]).astype(jnp.bfloat16)

        placed(rows, store)
        return carry

    def own_chunk(i, carry):
        to = pl.ds(pl.multiple_of(i * step, step), step)

        def store(nb, at, v):
            emb_ref[nb, to, at] = v.astype(jnp.bfloat16)

        placed(pl.ds(pl.multiple_of((own_ylo * 4 + z) * 64 + i * step, step), step), store)
        return carry

    @pl.when(pl.program_id(0) == 0)
    def _():
        copies = [
            pltpu.make_async_copy(blocks[r], all_ref.at[(own_ylo + r // 4) % 2 * 4 + (z + r) % 4], sems.at[r])
            for r in range(8)
        ]
        for copy in copies:
            copy.start()
        normed_ref[:, ROWS : ROWS + ACTS, :] = act_ref[...]
        for copy in copies:
            copy.wait()
        lax.fori_loop(0, ROWS // step, chunk, 0)
        lax.fori_loop(0, 2, own_chunk, 0)

    acc = None
    for p in range(0, 16, 4):
        part = jnp.dot(
            jnp.concatenate([normed_ref[block_of(p + i)] for i in range(4)], axis=1),
            jnp.concatenate([pieces[p + i][...] for i in range(4)], axis=0),
            preferred_element_type=jnp.float32,
        )
        acc = part if acc is None else acc + part
    out_ref[...] = acc.astype(jnp.bfloat16)


def project(gain, acts, blocks, pieces):
    width = pieces[0].shape[1]
    tile = 512
    return pl.pallas_call(
        project_kernel,
        grid=(width // tile,),
        in_specs=[VMEM, VMEM]
        + [ANY] * 8
        + [pl.BlockSpec((256, tile), lambda n: (0, n))] * 16,
        out_specs=[
            pl.BlockSpec((ROWS + ACTS, tile), lambda n: (0, n)),
            pl.BlockSpec((NB, 64, 256), lambda n: (0, 0, 0)),
        ],
        out_shape=[
            jax.ShapeDtypeStruct((ROWS + ACTS, width), jnp.bfloat16),
            jax.ShapeDtypeStruct((NB, 64, 256), jnp.bfloat16),
        ],
        scratch_shapes=[
            pltpu.VMEM((8, ROWS, 512), jnp.bfloat16),
            pltpu.VMEM((NB, ROWS + ACTS, 256), jnp.bfloat16),
            pltpu.SemaphoreType.DMA((8,)),
        ],
        compiler_params=LIMIT,
        name="project",
    )(gain, acts, *blocks, *pieces)


def attend_kernel(qkv_ref, own_ref, other_ref, out_ref):
    own_ylo = place()[2]
    inv_root = 1.0 / math.sqrt(HD)
    width = HEADS * HD
    half = P_SIZE // 2
    causal = [
        lax.broadcasted_iota(jnp.int32, (half, n), 0) + (n - half)
        >= lax.broadcasted_iota(jnp.int32, (half, n), 1)
        for n in (half, P_SIZE)
    ]
    row_frame = lax.broadcasted_iota(jnp.int32, (ACTS, P_SIZE), 0) // SLOTS
    i = lax.broadcasted_iota(jnp.int32, (ACTS, ACTS), 0)
    j = lax.broadcasted_iota(jnp.int32, (ACTS, ACTS), 1)
    seen = (i // SLOTS == j // SLOTS) & (j <= i)

    def patch_rows(frame, start):
        return jnp.concatenate(
            [
                qkv_ref[t * 64 + frame * 32 : t * 64 + frame * 32 + 32, start : start + HD]
                for t in range(8)
            ],
            axis=0,
        )

    def scores(a, b):
        s = lax.dot_general(a, b, (((1,), (1,)), ((), ())), preferred_element_type=jnp.float32)
        return s * inv_root

    for h in range(HEADS):
        at = h * HD
        keys = [patch_rows(f, width + at) for f in range(FRAMES)]
        values = [patch_rows(f, 2 * width + at) for f in range(FRAMES)]
        for f in range(FRAMES):
            queries = patch_rows(f, at)
            for i_half, n in enumerate((half, P_SIZE)):
                q = queries[i_half * half : (i_half + 1) * half]
                s = jnp.where(causal[i_half], scores(q, keys[f][:n]), -1e30)
                e = jnp.exp(s - jnp.max(s, axis=-1, keepdims=True))
                total = jnp.sum(e, axis=-1, keepdims=True)
                o = jnp.dot(
                    e.astype(jnp.bfloat16), values[f][:n], preferred_element_type=jnp.float32
                )
                o = (o * (1.0 / total)).astype(jnp.bfloat16)
                side = (own_ylo + i_half) % 2
                for t in range(4):
                    row = t * 64 + f * 32
                    out_ref[side, row : row + 32, at : at + HD] = o[t * 32 : (t + 1) * 32]
        rows = slice(ROWS, ROWS + ACTS)
        qa = qkv_ref[rows, at : at + HD]
        ka = qkv_ref[rows, width + at : width + at + HD]
        va = qkv_ref[rows, 2 * width + at : 2 * width + at + HD]
        parts = [jnp.where(row_frame == f, scores(qa, keys[f]), -1e30) for f in range(FRAMES)]
        own = jnp.where(seen, scores(qa, ka), -1e30)
        top = jnp.max(own, axis=-1, keepdims=True)
        for s in parts:
            top = jnp.maximum(top, jnp.max(s, axis=-1, keepdims=True))
        parts = [jnp.exp(s - top) for s in parts]
        own = jnp.exp(own - top)
        total = jnp.sum(own, axis=-1, keepdims=True)
        for e in parts:
            total = total + jnp.sum(e, axis=-1, keepdims=True)
        mixed = jnp.dot(own.astype(jnp.bfloat16), va, preferred_element_type=jnp.float32)
        for e, v in zip(parts, values):
            mixed = mixed + jnp.dot(
                e.astype(jnp.bfloat16), v, preferred_element_type=jnp.float32
            )
        mixed = mixed * (1.0 / total)
        for f in range(FRAMES):
            out_ref[(own_ylo + f) % 2, 256:264, at : at + HD] = mixed[
                f * SLOTS : (f + 1) * SLOTS
            ].astype(jnp.bfloat16)
    own_ref[...] = out_ref[0]
    other_ref[...] = out_ref[1]


def attend(qkv):
    shape = (264, HEADS * HD)
    return pl.pallas_call(
        attend_kernel,
        in_specs=[VMEM],
        out_specs=[VMEM, VMEM],
        out_shape=[jax.ShapeDtypeStruct(shape, jnp.bfloat16)] * 2,
        scratch_shapes=[pltpu.VMEM((2, *shape), jnp.bfloat16)],
        compiler_params=LIMIT,
        name="attend",
    )(qkv)


def expand_kernel(first, own_ref, other_ref, *refs):
    pieces, refs = refs[:8], refs[8:]
    act_ref, acc_ref = refs[-2:]
    outs = refs[-6:-2]
    if first == 0:
        act_ref[...] = jnp.zeros(act_ref.shape, act_ref.dtype)
    else:
        act_ref[...] = refs[0][...]
    mixed = jnp.concatenate([own_ref[...], other_ref[...]], axis=1)
    for p in range(8):
        acc = jnp.dot(mixed, pieces[p][...], preferred_element_type=jnp.float32)
        acc_ref[p % 2] = acc[:256].astype(jnp.bfloat16)
        act_ref[block_of(first + p)] = acc[256:264].astype(jnp.bfloat16)
        for b in range(4):
            rows = pl.ds(pl.multiple_of((place()[3] + b) % 4 * 64, 64), 64)
            outs[b][p] = acc_ref[p % 2, rows]


def expand(first, mixed, other, pieces, acts=()):
    return pl.pallas_call(
        functools.partial(expand_kernel, first),
        in_specs=[VMEM] * (10 + len(acts)),
        out_specs=[VMEM] * 5,
        out_shape=[jax.ShapeDtypeStruct((8, 64, 256), jnp.bfloat16)] * 4
        + [jax.ShapeDtypeStruct((NB, SLOTS, 256), jnp.bfloat16)],
        scratch_shapes=[pltpu.VMEM((2, 256, 256), jnp.bfloat16)],
        compiler_params=LIMIT,
    )(mixed, other, *pieces[first : first + 8], *acts)


def on_device(
    patches, teacher, proj_w, norm_gain, wq, wk, wv, wo, start_row, action_table, final_gain, head_w
):
    tensor = lax.axis_index("tensor")

    shard = proj_w.T
    both = jnp.concatenate([shard, get(shard, dyh=1)], axis=0)
    along = [both] + [get(both, dx=d) for d in (1, 2, 3)]
    columns = [s for near in along for s in (near, get(near, dc=1))]

    own = patches.reshape(64, V)
    rows = lax.all_to_all(
        jnp.broadcast_to(own[None], (8, 64, V)), "tensor", 0, 0, tiled=True
    ).reshape(ROWS, V)

    qkv_pieces = weight_pieces(join(wq, wk, wv))
    wo_pieces = weight_pieces(jnp.concatenate([wo, get(wo, dyl=1)], axis=0))

    acts, actions, gain = prepare(teacher, start_row, action_table, norm_gain)
    rows, acts, gain = lax.optimization_barrier((rows, acts, gain))
    embedded = embed(rows, columns)
    pair = (embedded, get(embedded, dyl=1))
    up = tuple(get(e, dz=1) for e in pair)
    down = tuple(get(e, dz=3) for e in pair)
    far = (get(up[0], dz=1), get(down[1], dz=3))
    blocks = [r[i] for i in range(2) for r in (pair, up, far, down)]

    qkv, embedded_own = project(gain, acts, blocks, qkv_pieces)
    mixed, other = attend(qkv)
    other = get(other, dyl=1)
    *shares, act_part = expand(0, mixed, other, wo_pieces)
    parts = [shares[0]] + [get(shares[b], dz=-b) for b in range(1, 4)]
    *shares, act_part = expand(8, mixed, other, wo_pieces, (act_part,))

    act_update = act_part.astype(jnp.float32)
    for b in range(1, 4):
        act_update = act_update + get(act_part, dz=b).astype(jnp.float32)
    parts += [shares[0]] + [get(shares[b], dz=-b) for b in range(1, 4)]
    ylo = tensor // 4
    act_update = jnp.transpose(act_update, (1, 0, 2)).reshape(SLOTS, D)
    acted = lax.dynamic_slice_in_dim(actions, ylo * SLOTS, SLOTS, 0) + act_update
    final = normalize(acted, final_gain).astype(jnp.bfloat16)
    logits = jnp.dot(final, head_w, preferred_element_type=jnp.float32)
    target = jnp.pad(lax.dynamic_slice_in_dim(teacher, ylo, 1, 0)[0], (0, 1))
    chosen = (target[:, None] == jnp.arange(BINS, dtype=jnp.int32)).astype(jnp.float32)
    picked = jnp.sum(logits * chosen, axis=-1)
    loss = jax.nn.logsumexp(logits, axis=-1) - picked
    return tuple(finish(loss, get(loss, dyl=1), embedded_own, parts))


def solution(mesh):
    return jax.shard_map(
        on_device,
        mesh=mesh,
        in_specs=(
            P(("dp", "section"), "tensor", None),
            P(("dp", "section"), None),
            P(None, ("dp", "tensor", "section")),
            P(),
            P(("dp", "section"), "tensor"),
            P(("dp", "section"), "tensor"),
            P(("dp", "section"), "tensor"),
            P("tensor", ("dp", "section")),
            P(),
            P(),
            P(),
            P(),
        ),
        out_specs=(P(("dp", "section"), "tensor", None), P(("dp", "section"), None)),
        check_vma=False,
    )
```

```python
import functools
import math

import jax
import jax.numpy as jnp
import numpy as np
from jax import lax
from jax.experimental import pallas as pl
from jax.experimental.pallas import tpu as pltpu
from jax.sharding import PartitionSpec as P


D = 4096
HD = 128
V = 1152
P_SIZE = 256
BINS = 256
ADIM = 7
SLOTS = 8
FRAMES = 2
ROWS = FRAMES * P_SIZE
ACTS = FRAMES * SLOTS
HEADS = 4
NB = 16

eps = 1e-05


AXES = ("dp", "tensor", "section")
IDS = np.arange(128).reshape(4, 2, 2, 4, 2)
VMEM = pl.BlockSpec(memory_space=pltpu.VMEM)
SMEM = pl.BlockSpec(memory_space=pltpu.SMEM)
ANY = pl.BlockSpec(memory_space=pl.ANY)
LIMIT = pltpu.CompilerParams(vmem_limit_bytes=56 * 1024 * 1024)


def get(s, dx=0, dc=0, dyl=0, dz=0, dyh=0):
    pairs = []
    for x, c, yl, z, yh in np.ndindex(IDS.shape):
        source = IDS[(x + dx) % 4, c ^ dc, yl ^ dyl, (z + dz) % 4, yh ^ dyh]
        pairs.append((int(source), int(IDS[x, c, yl, z, yh])))
    return lax.ppermute(s, AXES, pairs)


def place():
    dp, tensor = lax.axis_index("dp"), lax.axis_index("tensor")
    return dp // 2, dp % 2, tensor // 4, tensor % 4, lax.axis_index("section")


def block_of(p):
    x, core, _, _, yhi = place()
    return (x + p // 4) % 4 * 4 + (core + p // 2) % 2 * 2 + (yhi + p) % 2


def weight_pieces(shard):
    near = (shard, get(shard, dyh=1))
    ahead = tuple(get(s, dx=1) for s in near)
    behind = tuple(get(s, dx=3) for s in near)
    across = (get(ahead[0], dx=1), get(behind[1], dx=3))
    pieces = []
    for ring in (near, ahead, across, behind):
        pieces += list(ring)
        pieces += [get(s, dc=1) for s in ring]
    return pieces


def normalize(rows, gain):
    rows = rows.astype(jnp.float32)
    factor = lax.rsqrt(jnp.mean(rows * rows, axis=-1, keepdims=True) + eps)
    return rows * factor * gain.astype(jnp.float32)


def join_kernel(q_ref, k_ref, v_ref, out_ref):
    width = q_ref.shape[1]
    for n, ref in enumerate((q_ref, k_ref, v_ref)):
        out_ref[:, n * width : (n + 1) * width] = ref[...]


def join(q, k, v):
    return pl.pallas_call(
        join_kernel,
        in_specs=[VMEM] * 3,
        out_specs=VMEM,
        out_shape=jax.ShapeDtypeStruct((q.shape[0], 3 * q.shape[1]), jnp.bfloat16),
        name="join",
    )(q, k, v)


def prepare_kernel(tokens_ref, start_ref, rows_ref, gain_ref, acts_ref, actions_ref, gains_ref):
    tokens = tokens_ref[...]
    picks = jnp.where(tokens == lax.broadcasted_iota(jnp.int32, (ACTS, BINS), 1), 1.0, 0.0)
    looked = jnp.dot(
        picks.astype(jnp.bfloat16), rows_ref[...], preferred_element_type=jnp.float32
    )
    actions = jnp.where(tokens < 0, start_ref[...].astype(jnp.float32), looked)
    actions_ref[...] = actions
    gain = gain_ref[...].astype(jnp.float32)
    factor = lax.rsqrt(jnp.sum(actions * actions, axis=-1, keepdims=True) * (1.0 / D) + eps)
    normed = (actions * factor * gain).astype(jnp.bfloat16)
    for nb in range(NB):
        acts_ref[nb] = normed[:, nb * 256 : (nb + 1) * 256]
        gains_ref[nb] = gain[:, nb * 256 : (nb + 1) * 256]


def prepare(teacher, start_row, action_table, norm_gain):
    tokens = jnp.pad(teacher, ((0, 0), (1, 0)), constant_values=-1).reshape(ACTS, 1)
    return pl.pallas_call(
        prepare_kernel,
        in_specs=[VMEM] * 4,
        out_specs=[VMEM] * 3,
        out_shape=[
            jax.ShapeDtypeStruct((NB, ACTS, 256), jnp.bfloat16),
            jax.ShapeDtypeStruct((ACTS, D), jnp.float32),
            jax.ShapeDtypeStruct((NB, 1, 256), jnp.float32),
        ],
        compiler_params=LIMIT,
        name="prepare",
    )(tokens, start_row.reshape(1, D), action_table, norm_gain.reshape(1, D))


def finish_kernel(loss_ref, other_ref, emb_ref, *refs):
    parts, (out_ref, losses_ref) = refs[:8], refs[8:]
    own_ylo = place()[2]
    for a in range(ADIM):
        losses_ref[own_ylo, a] = loss_ref[a]
        losses_ref[1 - own_ylo, a] = other_ref[a]
    for p in range(NB):
        nb = block_of(p)
        of = [part[p % 8].astype(jnp.float32) for part in parts[p // 8 * 4 : p // 8 * 4 + 4]]
        update = (of[0] + of[1]) + (of[2] + of[3])
        total = (emb_ref[nb].astype(jnp.float32) + update).astype(jnp.bfloat16)
        cols = pl.ds(pl.multiple_of(nb * 256, 256), 256)
        for f in range(FRAMES):
            out_ref[f, :, cols] = total[f * 32 : (f + 1) * 32]


def finish(loss, other, embedded, parts):
    return pl.pallas_call(
        finish_kernel,
        in_specs=[SMEM] * 2 + [VMEM] * 9,
        out_specs=[VMEM, SMEM],
        out_shape=[
            jax.ShapeDtypeStruct((FRAMES, 32, D), jnp.bfloat16),
            jax.ShapeDtypeStruct((FRAMES, ADIM), jnp.float32),
        ],
        compiler_params=LIMIT,
        name="finish",
    )(loss, other, embedded, *parts)


def embed_kernel(*refs):
    rows, pieces, (out_ref, rows_ref, columns_ref) = refs[:8], refs[8:16], refs[16:]
    _, _, ylo, z, yhi = place()
    for r in range(8):
        t = (ylo + r // 4) % 2 * 4 + (z + r) % 4
        rows_ref[pl.ds(pl.multiple_of(t * 64, 64), 64), :] = rows[r][...]
    for p in range(8):
        for h in range(2):
            to = pl.ds(pl.multiple_of(p * 64 + (yhi + h) % 2 * 32, 32), 32)
            columns_ref[to, :] = pieces[p][h * 32 : (h + 1) * 32, :]
    out_ref[...] = lax.dot_general(
        rows_ref[...],
        columns_ref[...],
        (((1,), (1,)), ((), ())),
        preferred_element_type=jnp.float32,
    ).astype(jnp.bfloat16)


def embed(rows, pieces):
    return pl.pallas_call(
        embed_kernel,
        in_specs=[VMEM] * 16,
        out_specs=VMEM,
        out_shape=jax.ShapeDtypeStruct((ROWS, 512), jnp.bfloat16),
        scratch_shapes=[pltpu.VMEM((512, V), jnp.bfloat16)] * 2,
        compiler_params=LIMIT,
        name="embed",
    )(*rows, *pieces)


def project_kernel(gain_ref, act_ref, *refs):
    x, core, own_ylo, z, _ = place()
    blocks, pieces = refs[:8], refs[8:24]
    out_ref, emb_ref, all_ref, normed_ref, sems = refs[24:]
    step = 32
    low = lax.broadcasted_iota(jnp.int32, (step, 128), 1) < 64

    def placed(rows, store):
        for ylo in range(2):
            for pair in range(2):
                for m in range(4):
                    cols = slice(m * 128, (m + 1) * 128)
                    a = all_ref[ylo * 4 + pair * 2, rows, cols].astype(jnp.float32)
                    b = all_ref[ylo * 4 + pair * 2 + 1, rows, cols].astype(jnp.float32)
                    at = slice(pair * 128, (pair + 1) * 128)
                    even = jnp.where(low, a, pltpu.roll(b, 64, 1))
                    odd = jnp.where(low, pltpu.roll(a, 64, 1), b)
                    at_x = (x + m) % 4 * 4 + ylo
                    store(at_x + core * 2, at, even)
                    store(at_x + (1 - core) * 2, at, odd)

    def chunk(i, carry):
        rows = pl.ds(pl.multiple_of(i * step, step), step)
        totals = [jnp.zeros((step, 128), jnp.float32) for _ in range(4)]
        for t in range(8):
            for m in range(4):
                v = all_ref[t, rows, m * 128 : (m + 1) * 128].astype(jnp.float32)
                totals[m] = totals[m] + v * v
        total = (totals[0] + totals[1]) + (totals[2] + totals[3])
        mean = jnp.sum(total, axis=1, keepdims=True) * (1.0 / D)
        factor = jnp.broadcast_to(lax.rsqrt(mean + eps), (step, 128))

        def store(nb, at, v):
            normed_ref[nb, rows, at] = (v * factor * gain_ref[nb, :, at]).astype(jnp.bfloat16)

        placed(rows, store)
        return carry

    def own_chunk(i, carry):
        to = pl.ds(pl.multiple_of(i * step, step), step)

        def store(nb, at, v):
            emb_ref[nb, to, at] = v.astype(jnp.bfloat16)

        placed(pl.ds(pl.multiple_of((own_ylo * 4 + z) * 64 + i * step, step), step), store)
        return carry

    @pl.when(pl.program_id(0) == 0)
    def _():
        copies = [
            pltpu.make_async_copy(blocks[r], all_ref.at[(own_ylo + r // 4) % 2 * 4 + (z + r) % 4], sems.at[r])
            for r in range(8)
        ]
        for copy in copies:
            copy.start()
        normed_ref[:, ROWS : ROWS + ACTS, :] = act_ref[...]
        for copy in copies:
            copy.wait()
        lax.fori_loop(0, ROWS // step, chunk, 0)
        lax.fori_loop(0, 2, own_chunk, 0)

    acc = None
    for p in range(0, 16, 4):
        part = jnp.dot(
            jnp.concatenate([normed_ref[block_of(p + i)] for i in range(4)], axis=1),
            jnp.concatenate([pieces[p + i][...] for i in range(4)], axis=0),
            preferred_element_type=jnp.float32,
        )
        acc = part if acc is None else acc + part
    out_ref[...] = acc.astype(jnp.bfloat16)


def project(gain, acts, blocks, pieces):
    width = pieces[0].shape[1]
    tile = 512
    return pl.pallas_call(
        project_kernel,
        grid=(width // tile,),
        in_specs=[VMEM, VMEM]
        + [ANY] * 8
        + [pl.BlockSpec((256, tile), lambda n: (0, n))] * 16,
        out_specs=[
            pl.BlockSpec((ROWS + ACTS, tile), lambda n: (0, n)),
            pl.BlockSpec((NB, 64, 256), lambda n: (0, 0, 0)),
        ],
        out_shape=[
            jax.ShapeDtypeStruct((ROWS + ACTS, width), jnp.bfloat16),
            jax.ShapeDtypeStruct((NB, 64, 256), jnp.bfloat16),
        ],
        scratch_shapes=[
            pltpu.VMEM((8, ROWS, 512), jnp.bfloat16),
            pltpu.VMEM((NB, ROWS + ACTS, 256), jnp.bfloat16),
            pltpu.SemaphoreType.DMA((8,)),
        ],
        compiler_params=LIMIT,
        name="project",
    )(gain, acts, *blocks, *pieces)


def attend_kernel(qkv_ref, own_ref, other_ref, out_ref):
    own_ylo = place()[2]
    inv_root = 1.0 / math.sqrt(HD)
    width = HEADS * HD
    half = P_SIZE // 2
    causal = [
        lax.broadcasted_iota(jnp.int32, (half, n), 0) + (n - half)
        >= lax.broadcasted_iota(jnp.int32, (half, n), 1)
        for n in (half, P_SIZE)
    ]
    row_frame = lax.broadcasted_iota(jnp.int32, (ACTS, P_SIZE), 0) // SLOTS
    i = lax.broadcasted_iota(jnp.int32, (ACTS, ACTS), 0)
    j = lax.broadcasted_iota(jnp.int32, (ACTS, ACTS), 1)
    seen = (i // SLOTS == j // SLOTS) & (j <= i)

    def patch_rows(frame, start):
        return jnp.concatenate(
            [
                qkv_ref[t * 64 + frame * 32 : t * 64 + frame * 32 + 32, start : start + HD]
                for t in range(8)
            ],
            axis=0,
        )

    def scores(a, b):
        s = lax.dot_general(a, b, (((1,), (1,)), ((), ())), preferred_element_type=jnp.float32)
        return s * inv_root

    for h in range(HEADS):
        at = h * HD
        keys = [patch_rows(f, width + at) for f in range(FRAMES)]
        values = [patch_rows(f, 2 * width + at) for f in range(FRAMES)]
        for f in range(FRAMES):
            queries = patch_rows(f, at)
            for i_half, n in enumerate((half, P_SIZE)):
                q = queries[i_half * half : (i_half + 1) * half]
                s = jnp.where(causal[i_half], scores(q, keys[f][:n]), -1e30)
                e = jnp.exp(s - jnp.max(s, axis=-1, keepdims=True))
                total = jnp.sum(e, axis=-1, keepdims=True)
                o = jnp.dot(
                    e.astype(jnp.bfloat16), values[f][:n], preferred_element_type=jnp.float32
                )
                o = (o * (1.0 / total)).astype(jnp.bfloat16)
                side = (own_ylo + i_half) % 2
                for t in range(4):
                    row = t * 64 + f * 32
                    out_ref[side, row : row + 32, at : at + HD] = o[t * 32 : (t + 1) * 32]
        rows = slice(ROWS, ROWS + ACTS)
        qa = qkv_ref[rows, at : at + HD]
        ka = qkv_ref[rows, width + at : width + at + HD]
        va = qkv_ref[rows, 2 * width + at : 2 * width + at + HD]
        parts = [jnp.where(row_frame == f, scores(qa, keys[f]), -1e30) for f in range(FRAMES)]
        own = jnp.where(seen, scores(qa, ka), -1e30)
        top = jnp.max(own, axis=-1, keepdims=True)
        for s in parts:
            top = jnp.maximum(top, jnp.max(s, axis=-1, keepdims=True))
        parts = [jnp.exp(s - top) for s in parts]
        own = jnp.exp(own - top)
        total = jnp.sum(own, axis=-1, keepdims=True)
        for e in parts:
            total = total + jnp.sum(e, axis=-1, keepdims=True)
        mixed = jnp.dot(own.astype(jnp.bfloat16), va, preferred_element_type=jnp.float32)
        for e, v in zip(parts, values):
            mixed = mixed + jnp.dot(
                e.astype(jnp.bfloat16), v, preferred_element_type=jnp.float32
            )
        mixed = mixed * (1.0 / total)
        for f in range(FRAMES):
            out_ref[(own_ylo + f) % 2, 256:264, at : at + HD] = mixed[
                f * SLOTS : (f + 1) * SLOTS
            ].astype(jnp.bfloat16)
    own_ref[...] = out_ref[0]
    other_ref[...] = out_ref[1]


def attend(qkv):
    shape = (264, HEADS * HD)
    return pl.pallas_call(
        attend_kernel,
        in_specs=[VMEM],
        out_specs=[VMEM, VMEM],
        out_shape=[jax.ShapeDtypeStruct(shape, jnp.bfloat16)] * 2,
        scratch_shapes=[pltpu.VMEM((2, *shape), jnp.bfloat16)],
        compiler_params=LIMIT,
        name="attend",
    )(qkv)


def expand_kernel(first, own_ref, other_ref, *refs):
    pieces, refs = refs[:8], refs[8:]
    act_ref, acc_ref = refs[-2:]
    outs = refs[-6:-2]
    if first == 0:
        act_ref[...] = jnp.zeros(act_ref.shape, act_ref.dtype)
    else:
        act_ref[...] = refs[0][...]
    mixed = jnp.concatenate([own_ref[...], other_ref[...]], axis=1)
    for p in range(8):
        acc = jnp.dot(mixed, pieces[p][...], preferred_element_type=jnp.float32)
        acc_ref[p % 2] = acc[:256].astype(jnp.bfloat16)
        act_ref[block_of(first + p)] = acc[256:264].astype(jnp.bfloat16)
        for b in range(4):
            rows = pl.ds(pl.multiple_of((place()[3] + b) % 4 * 64, 64), 64)
            outs[b][p] = acc_ref[p % 2, rows]


def expand(first, mixed, other, pieces, acts=()):
    return pl.pallas_call(
        functools.partial(expand_kernel, first),
        in_specs=[VMEM] * (10 + len(acts)),
        out_specs=[VMEM] * 5,
        out_shape=[jax.ShapeDtypeStruct((8, 64, 256), jnp.bfloat16)] * 4
        + [jax.ShapeDtypeStruct((NB, SLOTS, 256), jnp.bfloat16)],
        scratch_shapes=[pltpu.VMEM((2, 256, 256), jnp.bfloat16)],
        compiler_params=LIMIT,
    )(mixed, other, *pieces[first : first + 8], *acts)


def on_device(
    patches, teacher, proj_w, norm_gain, wq, wk, wv, wo, start_row, action_table, final_gain, head_w
):
    tensor = lax.axis_index("tensor")

    shard = proj_w.T
    both = jnp.concatenate([shard, get(shard, dyh=1)], axis=0)
    along = [both] + [get(both, dx=d) for d in (1, 2, 3)]
    columns = [s for near in along for s in (near, get(near, dc=1))]

    own = patches.reshape(64, V)
    swapped = get(own, dyl=1)
    rows = [get(r, dz=b) if b else r for r in (own, swapped) for b in range(4)]

    qkv_pieces = weight_pieces(join(wq, wk, wv))
    wo_pieces = weight_pieces(jnp.concatenate([wo, get(wo, dyl=1)], axis=0))

    acts, actions, gain = prepare(teacher, start_row, action_table, norm_gain)
    embedded = embed(rows, columns)
    pair = (embedded, get(embedded, dyl=1))
    up = tuple(get(e, dz=1) for e in pair)
    down = tuple(get(e, dz=3) for e in pair)
    far = (get(up[0], dz=1), get(down[1], dz=3))
    blocks = [r[i] for i in range(2) for r in (pair, up, far, down)]

    qkv, embedded_own = project(gain, acts, blocks, qkv_pieces)
    mixed, other = attend(qkv)
    other = get(other, dyl=1)
    *shares, act_part = expand(0, mixed, other, wo_pieces)
    parts = [shares[0]] + [get(shares[b], dz=-b) for b in range(1, 4)]
    *shares, act_part = expand(8, mixed, other, wo_pieces, (act_part,))

    act_update = act_part.astype(jnp.float32)
    for b in range(1, 4):
        act_update = act_update + get(act_part, dz=b).astype(jnp.float32)
    parts += [shares[0]] + [get(shares[b], dz=-b) for b in range(1, 4)]
    ylo = tensor // 4
    act_update = jnp.transpose(act_update, (1, 0, 2)).reshape(SLOTS, D)
    acted = lax.dynamic_slice_in_dim(actions, ylo * SLOTS, SLOTS, 0) + act_update
    final = normalize(acted, final_gain).astype(jnp.bfloat16)
    logits = jnp.dot(final, head_w, preferred_element_type=jnp.float32)
    target = jnp.pad(lax.dynamic_slice_in_dim(teacher, ylo, 1, 0)[0], (0, 1))
    chosen = (target[:, None] == jnp.arange(BINS, dtype=jnp.int32)).astype(jnp.float32)
    picked = jnp.sum(logits * chosen, axis=-1)
    loss = jax.nn.logsumexp(logits, axis=-1) - picked
    return tuple(finish(loss, get(loss, dyl=1), embedded_own, parts))


def solution(mesh):
    return jax.shard_map(
        on_device,
        mesh=mesh,
        in_specs=(
            P(("dp", "section"), "tensor", None),
            P(("dp", "section"), None),
            P(None, ("dp", "tensor", "section")),
            P(),
            P(("dp", "section"), "tensor"),
            P(("dp", "section"), "tensor"),
            P(("dp", "section"), "tensor"),
            P("tensor", ("dp", "section")),
            P(),
            P(),
            P(),
            P(),
        ),
        out_specs=(P(("dp", "section"), "tensor", None), P(("dp", "section"), None)),
        check_vma=False,
    )
```
